32 devices in a mesh: lat: 8 (over z, x), lon: 4 (over y, core).
Axes of the slice: x: 2, y: 2, z: 4, core: 2. Of those that a mesh axis runs over, the one named last changes fastest.
Arguments:
- state: bfloat16 [2, 48, 96, 192], P(None, 'lat', 'lon'), may hold values from -6 to 6
- out_cot: bfloat16 [2, 48, 96, 192], P(None, 'lat', 'lon'), may hold values from -6 to 6
- qkv_weight: bfloat16 [2, 192, 576], replicated, may hold values from -0.4375 to 0.4375
- proj_weight: bfloat16 [2, 192, 192], replicated, may hold values from -0.4375 to 0.4375
- fc1_weight: bfloat16 [2, 192, 768], replicated, may hold values from -0.4375 to 0.4375
- fc2_weight: bfloat16 [2, 768, 192], replicated, may hold values from -0.21875 to 0.21875
- norm_gain: float32 [2, 2, 192], replicated, may hold values from 0.5 to 1.5
- bias_table: float32 [2, 8, 1, 6, 3312], P(None, 'lat'), may hold values from -3 to 303
Outputs:
- state_grad: float32 [2, 48, 96, 192], P(None, 'lat', 'lon')
- qkv_grad: float32 [2, 192, 576], P(None, 'lat', 'lon')
- proj_grad: float32 [2, 192, 192], P(None, 'lat', 'lon')
- fc1_grad: float32 [2, 192, 768], P(None, 'lat', 'lon')
- fc2_grad: float32 [2, 768, 192], P(None, 'lat', 'lon')
- norm_gain_grad: float32 [2, 2, 192], replicated
- bias_table_grad: float32 [2, 8, 1, 6, 3312], P(None, 'lat', None, None, 'lon')
The draws below stay inside these ranges and needn't reach their ends.
All inputs are finite; a program needn't handle non-finite values.
Results may differ from the reference program's by a relative error of at most 0.028.
Values may be sent and summed in bfloat16 or wider, within the bound.
No kernel may reach another device: no remote copies, remote signals or barrier semaphores. Data moves between devices by JAX's collectives and lax.ppermute only.
A program may use at most 128 MiB of HBM per device.

```python
import jax
import jax.numpy as jnp
from jax import lax

C = 192
HEADS = 6
HID = 768
Z = 2
WZ = 2
WH = 6
WW = 12
LAT = 48
LON = 96
NLATWIN = 8
ZWIN = 1
POS = 3312


def draw_bias_table(key, part):
    keys = jax.random.split(jax.random.fold_in(key, 17), 1)
    shape = (2, NLATWIN, ZWIN, HEADS, POS)
    return jnp.clip(jax.random.normal(keys[0], shape, jnp.float32), -3.0, 3.0)


def shard_levels(own_key, dims, cuts, low, top_value):
    def one(position, shards_of):
        draws = jax.random.uniform(jax.random.fold_in(jax.random.fold_in(own_key, 6), position), (shards_of,), jnp.float32, low / len(cuts), top_value / len(cuts))
        return jnp.repeat(jnp.exp(draws), dims[position] // shards_of).reshape((-1,) + (1,) * (len(dims) - position - 1))

    factor_of = one(*cuts[0])
    for cut in cuts[1:]:
        factor_of = factor_of * one(*cut)
    return factor_of


def scatter_about(rng, extent, spread, most, cuts=(), kind=jnp.bfloat16):
    values = jax.random.normal(rng, extent, jnp.float32) * spread
    if len(cuts) > 0:
        values = shard_levels(rng, extent, cuts, -0.22, 0.18) * values
    return jnp.clip(values, min=-most, max=most).astype(kind)


def setup_inputs(seed: int = 0) -> dict:
    streams_of = jax.random.split(jax.random.key(seed), 9)
    state = scatter_about(streams_of[0], (Z, LAT, LON, C), 1.0, 6.0, ((1, 8), (2, 4)))
    out_cot = scatter_about(streams_of[1], (Z, LAT, LON, C), 1.0, 6.0, ((1, 8), (2, 4)))
    qkv_weight = scatter_about(streams_of[2], (2, C, 3 * C), C ** -0.5, 0.4375)
    proj_weight = scatter_about(streams_of[3], (2, C, C), C ** -0.5, 0.4375)
    fc1_weight = scatter_about(streams_of[4], (2, C, HID), C ** -0.5, 0.4375)
    fc2_weight = scatter_about(streams_of[5], (2, HID, C), HID ** -0.5, 0.21875)
    norm_gain = jnp.clip(1.0 + 0.1 * jax.random.normal(streams_of[6], (2, 2, C), jnp.float32), 0.5, 1.5)
    bias_table = draw_bias_table(jax.random.fold_in(streams_of[8], 71), 0)
    return {"state": state, "out_cot": out_cot, "qkv_weight": qkv_weight, "proj_weight": proj_weight, "fc1_weight": fc1_weight, "fc2_weight": fc2_weight, "norm_gain": norm_gain, "bias_table": bias_table}


def position_index():
    tokens = jnp.arange(WZ * WH * WW, dtype=jnp.int32)
    level_in = tokens // (WH * WW)
    row_in = tokens // WW % WH
    column_in = tokens % WW
    level_part = (level_in[:, None] * WZ + level_in[None, :]) * (WH * WH * (2 * WW - 1))
    row_part = (row_in[:, None] * WH + row_in[None, :]) * (2 * WW - 1)
    return (level_part + row_part + column_in[:, None] - column_in[None, :] + WW - 1).astype(jnp.int32)

def shifted_labels(lat_windows, level_windows, lat_start, lat_total):
    tokens = jnp.arange(WZ * WH * WW, dtype=jnp.int32)
    level_in = tokens // (WH * WW)
    row_in = tokens // WW % WH
    global_level = jnp.arange(level_windows, dtype=jnp.int32)[None, :, None] * WZ + level_in[None, None, :]
    global_row = lat_start + jnp.arange(lat_windows, dtype=jnp.int32)[:, None, None] * WH + row_in[None, None, :]
    level_mark = (global_level >= level_windows * WZ - 1).astype(jnp.int32)
    row_mark = (global_row >= lat_total - WH // 2).astype(jnp.int32)
    return (2 * level_mark + row_mark).astype(jnp.int32)

def to_windows(brick):
    levels, rows, columns, model_width = brick.shape
    shaped = brick.reshape(levels // WZ, WZ, rows // WH, WH, columns // WW, WW, model_width)
    shaped = shaped.transpose(2, 0, 4, 1, 3, 5, 6)
    return shaped.reshape(rows // WH, levels // WZ, columns // WW, WZ * WH * WW, model_width)

def from_windows(windows):
    lat_windows, level_windows, lon_windows, window_size, model_width = windows.shape
    shaped = windows.reshape(lat_windows, level_windows, lon_windows, WZ, WH, WW, model_width)
    shaped = shaped.transpose(1, 3, 0, 4, 2, 5, 6)
    return shaped.reshape(level_windows * WZ, lat_windows * WH, lon_windows * WW, model_width)

def layer_norm(values, gain):
    average = lax.optimization_barrier(jnp.mean(values, -1, keepdims=True))
    centred = values - average
    variance = lax.optimization_barrier(jnp.mean(centred * centred, -1, keepdims=True))
    return centred * lax.rsqrt(variance + 1e-05) * gain

def rounded(values):
    return lax.optimization_barrier(values.astype(jnp.bfloat16)).astype(jnp.float32)

def run_block(values, gain_pair, table_part, offsets, labels, weights):
    w_qkv, w_proj, w_fc1, w_fc2 = weights
    head_count = table_part.shape[2]
    model_width = values.shape[-1]
    head_size = model_width // head_count
    normed = layer_norm(values, gain_pair[0]).astype(jnp.bfloat16)
    qkv_out = jnp.dot(normed, w_qkv, preferred_element_type=jnp.float32) + offsets[0]
    projected = rounded(qkv_out).reshape(values.shape[:-1] + (3, head_count, head_size))
    queries = projected[..., 0, :, :]
    key_vectors = projected[..., 1, :, :]
    value_vectors = projected[..., 2, :, :]
    scores = jnp.einsum('abcqhd,abckhd->abchqk', queries, key_vectors) * head_size ** (-0.5)
    bias_full = jnp.take(table_part, position_index(), axis=3)
    allowed = (labels[:, :, :, None] == labels[:, :, None, :])[:, :, None, None]
    scores = jnp.where(allowed, scores + bias_full[:, :, None], -1e+30)
    attention = rounded(jax.nn.softmax(scores, axis=-1))
    attended = jnp.einsum('abchqk,abckhd->abcqhd', attention, value_vectors).reshape(values.shape)
    joined = attended.astype(jnp.bfloat16)
    middle = values + jnp.dot(joined, w_proj, preferred_element_type=jnp.float32) + offsets[1]
    normed_two = layer_norm(middle, gain_pair[1]).astype(jnp.bfloat16)
    expanded = jnp.dot(normed_two, w_fc1, preferred_element_type=jnp.float32) + offsets[2]
    hidden = jax.nn.gelu(expanded, approximate=False).astype(jnp.bfloat16)
    result = middle + jnp.dot(hidden, w_fc2, preferred_element_type=jnp.float32) + offsets[3]
    return (result, (normed, joined, normed_two, hidden))

def open_block(values, gain_pair, table_part, labels, weights):
    lead = values.shape[:-1]
    model_width = values.shape[-1]
    offsets = (jnp.zeros(lead + (3 * model_width,), jnp.float32), jnp.zeros(lead + (model_width,), jnp.float32), jnp.zeros(lead + (weights[2].shape[1],), jnp.float32), jnp.zeros(lead + (model_width,), jnp.float32))

    def forward(inputs, gains_in, table_in, offsets_in):
        return run_block(inputs, gains_in, table_in, offsets_in, labels, weights)
    return jax.vjp(forward, values, gain_pair, table_part, offsets, has_aux=True)

def close_block(pullback, stored, cotangent):
    value_grad, gain_grad, table_grad, output_grads = pullback(cotangent)
    weight_grads = tuple((lax.dot_general(inputs_act.reshape(-1, inputs_act.shape[-1]), grad_out.reshape(-1, grad_out.shape[-1]).astype(jnp.bfloat16), (((0,), (0,)), ((), ())), preferred_element_type=jnp.float32) for inputs_act, grad_out in zip(stored, output_grads)))
    return (value_grad, weight_grads, gain_grad, table_grad)

def stripe_grads(values, cotangents, gain_pair, table_part, labels, weights):

    def one_stripe(carry, stripe):
        piece, cotangent, table_row, label_row = stripe
        result, pullback, stored = open_block(piece[None], gain_pair, table_row[None], label_row[None], weights)
        value_grad, weight_grads, gain_grad, table_grad = close_block(pullback, stored, cotangent[None])
        summed = tuple((left + right for left, right in zip(carry[0], weight_grads)))
        return ((summed, carry[1] + gain_grad), (value_grad[0], table_grad[0]))
    initial = (tuple((jnp.zeros(w.shape, jnp.float32) for w in weights)), jnp.zeros(gain_pair.shape, jnp.float32))
    (weight_grads, gain_grad), (value_grad, table_grad) = lax.scan(one_stripe, initial, (values, cotangents, table_part, labels))
    return (value_grad, weight_grads, gain_grad, table_grad)

def reference(state, out_cot, qkv_weight, proj_weight, fc1_weight, fc2_weight, norm_gain, bias_table):
    matrices = (qkv_weight, proj_weight, fc1_weight, fc2_weight)
    first_weights = tuple((w[0] for w in matrices))
    second_weights = tuple((w[1] for w in matrices))
    windows_in = to_windows(state.astype(jnp.float32))
    unmasked = jnp.zeros((NLATWIN, ZWIN, WZ * WH * WW), jnp.int32)

    def forward_stripe(stripe):
        piece, table_row, label_row = stripe
        result = open_block(piece[None], norm_gain[0], table_row[None], label_row[None], first_weights)[0]
        return result[0]
    first_out = lax.map(forward_stripe, (windows_in, bias_table[0], unmasked))
    state_one = from_windows(first_out).astype(jnp.bfloat16)
    shifts = (-(WZ // 2), -(WH // 2), -(WW // 2))
    rolled = jnp.roll(state_one, shifts, (0, 1, 2)).astype(jnp.float32)
    cot_rolled = jnp.roll(out_cot, shifts, (0, 1, 2)).astype(jnp.float32)
    shifted = shifted_labels(NLATWIN, ZWIN, 0, LAT)
    rolled_grad, second_grads, second_gains, second_table = stripe_grads(to_windows(rolled), to_windows(cot_rolled), norm_gain[1], bias_table[1], shifted, second_weights)
    state_one_grad = jnp.roll(from_windows(rolled_grad), (WZ // 2, WH // 2, WW // 2), (0, 1, 2))
    state_grad, first_grads, first_gains, first_table = stripe_grads(windows_in, to_windows(state_one_grad), norm_gain[0], bias_table[0], unmasked, first_weights)
    stacked = tuple((jnp.stack((left, right)) for left, right in zip(first_grads, second_grads)))
    return (from_windows(state_grad), stacked[0], stacked[1], stacked[2], stacked[3], jnp.stack((first_gains, second_gains)), jnp.stack((first_table, second_table)))
```

```python
import functools

import jax
import jax.numpy as jnp
import numpy as np
from jax import lax
from jax.experimental import pallas as pl
from jax.experimental.pallas import tpu as pltpu
from jax.sharding import PartitionSpec as P

WZ = 2
WH = 6
WW = 12
ZH = WZ * WH
SPAN = 2 * WW - 1
WT = ZH * WW
EPS = 1e-05
NEG = -1e30

f32 = jnp.float32
bf16 = jnp.bfloat16


def one_hot(sources, width):
    table = np.zeros((len(sources), width), np.float32)
    for row, source in enumerate(sources):
        if source >= 0:
            table[row, source] = 1.0
    return jnp.asarray(table, bf16)


class Plan:
    def __init__(self, lon, heads, channels):
        half_h, half_w = WH // 2, WW // 2
        self.lon, self.heads, self.channels = lon, heads, channels
        self.tokens = lon * ZH
        self.windows = lon // WW
        order = [(l, z, h) for l in range(lon) for z in range(WZ) for h in range(WH)]
        self.index = {t: i for i, t in enumerate(order)}
        natural = {(l, z, h): (z * WH + h) * lon + l for l, z, h in order}
        self.to_order = one_hot([natural[t] for t in order], self.tokens)
        place = {natural[t]: i for i, t in enumerate(order)}
        self.to_natural = one_hot([place[i] for i in range(self.tokens)], self.tokens)
        lat_msg = [t for t in order if t[2] < half_h and t[0] >= half_w]
        lon_msg = [t for t in order if t[2] >= half_h and t[0] < half_w]
        cor_msg = [t for t in order if t[2] < half_h and t[0] < half_w]
        self.sizes = (len(lat_msg), len(lon_msg), len(cor_msg))
        self.send_down = [one_hot([self.index[t] for t in m], self.tokens) for m in (lat_msg, lon_msg, cor_msg)]
        picks = ([], [], [], [])
        for l, z, h in order:
            t = (l + half_w, (z + WZ // 2) % WZ, h + half_h)
            over_l, over_h = t[0] >= lon, t[2] >= WH
            t = (t[0] % lon, t[1], t[2] % WH)
            which = {(False, False): 0, (False, True): 1, (True, False): 2, (True, True): 3}[(over_l, over_h)]
            source = self.index[t] if which == 0 else (lat_msg, lon_msg, cor_msg)[which - 1].index(t)
            for i, pick in enumerate(picks):
                pick.append(source if i == which else -1)
        self.roll = [one_hot(picks[0], self.tokens)] + [one_hot(p, n) for p, n in zip(picks[1:], self.sizes)]
        back = {}
        for l, z, h in order:
            t = (l + half_w, (z + WZ // 2) % WZ, h + half_h)
            which = {(False, False): 0, (False, True): 1, (True, False): 2, (True, True): 3}[(t[0] >= lon, t[2] >= WH)]
            back[(t[0] % lon, t[1], t[2] % WH)] = (which, self.index[(l, z, h)])
        msgs = ([], [], [])
        picks = ([], [], [], [])
        for t in order:
            which, source = back[t]
            if which:
                msgs[which - 1].append(source)
            for i, pick in enumerate(picks):
                pick.append((source if which == 0 else len(msgs[which - 1]) - 1) if i == which else -1)
        self.send_up = [one_hot(m, self.tokens) for m in msgs]
        self.unroll = [one_hot(picks[0], self.tokens)] + [one_hot(p, n) for p, n in zip(picks[1:], self.sizes)]
        row = -np.ones(16 * heads, np.int64)
        for h in range(heads):
            for i in range(ZH):
                row[16 * h + i] = 8 * i + h
        self.row_pick = one_hot(row, 8 * ZH)
        lane = -np.ones(384, np.int64)
        for d in range(SPAN):
            for zk in range(WZ):
                for hk in range(WH):
                    lane[(SPAN - 1 - d) * ZH + zk * WH + hk] = zk * 256 + hk * SPAN + d
        self.lane_pick = one_hot(lane, 512).T
        level = np.array([(r % ZH) // WH for r in range(WT)])
        late = np.array([int(r % WH >= WH // 2) for r in range(WT)])
        self.level_mask = jnp.asarray(np.where(level[:, None] == level[None, :], 0.0, NEG), f32)
        self.late_mask = jnp.asarray(np.where(late[:, None] == late[None, :], 0.0, NEG), f32)


def mm(a, b):
    return lax.dot_general(a, b, (((1,), (0,)), ((), ())), preferred_element_type=f32)


def mm_nt(a, b):
    return lax.dot_general(a, b, (((1,), (1,)), ((), ())), preferred_element_type=f32)


def mm_tn(a, b):
    return lax.dot_general(a, b, (((0,), (0,)), ((), ())), preferred_element_type=f32)


def split3(v):
    hi = v.astype(bf16)
    rest = v - hi.astype(f32)
    mid = rest.astype(bf16)
    low = (rest - mid.astype(f32)).astype(bf16)
    return hi, mid, low


def norm(u, gain):
    average = jnp.mean(u, -1, keepdims=True)
    centred = u - average
    scale = lax.rsqrt(jnp.mean(centred * centred, -1, keepdims=True) + EPS)
    hat = centred * scale
    return (hat * gain).astype(bf16), hat, scale


def norm_back(grad, hat, scale, gain):
    inner = grad * gain
    gain_grad = jnp.sum(grad * hat, 0, keepdims=True)
    value = scale * (inner - jnp.mean(inner, -1, keepdims=True) - hat * jnp.mean(inner * hat, -1, keepdims=True))
    return value, gain_grad


def expand_bias(block, table_ref, row_pick, lane_pick, x_ref, bias_ref, heads, mask):
    x_ref[...] = jnp.zeros_like(x_ref)
    table = table_ref[block]
    piece = WH * SPAN
    for i in range(ZH):
        for zk in range(WZ):
            zq, hq = i // WH, i % WH
            start = ((zq * WZ + zk) * WH + hq) * piece
            x_ref[8 * i : 8 * i + heads, 256 * zk : 256 * zk + piece] = table[:, start : start + piece]
    wide = None
    for part in split3(x_ref[...]):
        moved = mm(mm(row_pick[...], part).astype(bf16), lane_pick[...])
        wide = moved if wide is None else wide + moved
    for w in range(WW):
        start = (WW - 1 - w) * ZH
        turned = pltpu.roll(wide, (384 - start) % 384, 1) if start else wide
        for h in range(heads):
            rows = turned[16 * h : 16 * h + ZH, 0:WT]
            if mask is not None:
                rows = rows + mask[ZH * w : ZH * w + ZH, :]
            bias_ref[h, ZH * w : ZH * w + ZH, :] = rows


def fold_bias(bias_grad_ref, row_pick, lane_pick, fold_ref, out_ref, heads):
    fold_ref[...] = jnp.zeros_like(fold_ref)
    total = None
    for w in range(WW):
        for h in range(heads):
            fold_ref[16 * h : 16 * h + ZH, 0:WT] = bias_grad_ref[h, ZH * w : ZH * w + ZH, :]
        start = (WW - 1 - w) * ZH
        turned = fold_ref[...]
        if start:
            turned = pltpu.roll(turned, start, 1)
        total = turned if total is None else total + turned
    back = mm_nt(mm_tn(row_pick[...], total.astype(bf16)).astype(bf16), lane_pick[...])
    piece = WH * SPAN
    for i in range(ZH):
        for zk in range(WZ):
            zq, hq = i // WH, i % WH
            slot = (zq * WZ + zk) * WH + hq
            out_ref[slot] = back[8 * i : 8 * i + heads, 256 * zk : 256 * zk + piece].astype(out_ref.dtype)


def head_masks(heads, channels):
    lanes = lax.broadcasted_iota(jnp.int32, (1, channels), 1)
    size = channels // heads
    return [(lanes >= size * h) & (lanes < size * (h + 1)) for h in range(heads)]


def pick(mask, value):
    return jnp.where(mask, value, jnp.zeros_like(value))


def forward(u, block, gains, w, bias_ref, p_ref, plan):
    channels, heads = plan.channels, plan.heads
    w_qkv, w_proj, w_fc1, w_fc2 = w
    gain_one = gains[block, 0:1, :]
    gain_two = gains[block, 1:2, :]
    n1, hat1, scale1 = norm(u, gain_one)
    qkv_w = w_qkv[block]
    q, k, v = (mm(n1, qkv_w[:, i * channels : (i + 1) * channels]).astype(bf16) for i in range(3))
    masks = head_masks(heads, channels)
    factor = (channels // heads) ** (-0.5)
    outs = []
    for n in range(plan.windows):
        rows = slice(n * WT, (n + 1) * WT)
        qw, kw, vw = q[rows], k[rows], v[rows]
        total = None
        for h in range(heads):
            s = mm_nt(pick(masks[h], qw), kw) * factor + bias_ref[h]
            e = jnp.exp(s - jnp.max(s, -1, keepdims=True))
            p = (e / jnp.sum(e, -1, keepdims=True))
            if p_ref is not None:
                p_ref[n * heads + h] = p
            o = mm(p.astype(bf16), pick(masks[h], vw))
            total = o if total is None else total + o
        outs.append(total.astype(bf16))
    o = jnp.concatenate(outs, 0)
    middle = u + mm(o, w_proj[block])
    n2, hat2, scale2 = norm(middle, gain_two)
    wide = mm(n2, w_fc1[block])
    cdf = 0.5 * (1.0 + lax.erf(wide * (0.5**0.5)))
    g = (wide * cdf).astype(bf16)
    out = middle + mm(g, w_fc2[block])
    return out, (n1, hat1, scale1, q, k, v, o, n2, hat2, scale2, wide, cdf, g)


def backward(grad, kept, block, gains, w, bias_grad_ref, p_ref, plan):
    channels, heads = plan.channels, plan.heads
    w_qkv, w_proj, w_fc1, w_fc2 = w
    n1, hat1, scale1, q, k, v, o, n2, hat2, scale2, wide, cdf, g = kept
    gain_one = gains[block, 0:1, :]
    gain_two = gains[block, 1:2, :]
    dz = grad.astype(bf16)
    dg = mm_nt(dz, w_fc2[block]).astype(bf16).astype(f32)
    density = jnp.exp(-0.5 * wide * wide) * (1.0 / np.sqrt(2.0 * np.pi))
    dh = (dg * (cdf + wide * density)).astype(bf16)
    dn2 = mm_nt(dh, w_fc1[block]).astype(bf16).astype(f32)
    dmid, gain_grad_two = norm_back(dn2, hat2, scale2, gain_two)
    dmid = grad + dmid
    dp_out = dmid.astype(bf16)
    do = mm_nt(dp_out, w_proj[block]).astype(bf16)
    masks = head_masks(heads, channels)
    factor = (channels // heads) ** (-0.5)
    dqs, dks, dvs = [], [], []
    for n in range(plan.windows):
        rows = slice(n * WT, (n + 1) * WT)
        qw, kw, vw, dow = q[rows], k[rows], v[rows], do[rows]
        dq = dk = dv = None
        for h in range(heads):
            dom = pick(masks[h], dow)
            p = p_ref[n * heads + h]
            dp = mm_nt(dom, vw).astype(bf16).astype(f32)
            ds = p * (dp - jnp.sum(dp * p, -1, keepdims=True))
            if n == 0:
                bias_grad_ref[h] = ds
            else:
                bias_grad_ref[h] += ds
            dsb = (ds * factor).astype(bf16)
            a = mm(dsb, pick(masks[h], kw))
            b = mm_tn(dsb, pick(masks[h], qw))
            c = mm_tn(p.astype(bf16), dom)
            dq, dk, dv = (a, b, c) if dq is None else (dq + a, dk + b, dv + c)
        dqs.append(dq.astype(bf16))
        dks.append(dk.astype(bf16))
        dvs.append(dv.astype(bf16))
    dq, dk, dv = (jnp.concatenate(parts, 0) for parts in (dqs, dks, dvs))
    qkv_w = w_qkv[block]
    dn1 = None
    for i, part in enumerate((dq, dk, dv)):
        term = mm_nt(part, qkv_w[:, i * channels : (i + 1) * channels])
        dn1 = term if dn1 is None else dn1 + term
    dn1 = dn1.astype(bf16).astype(f32)
    du, gain_grad_one = norm_back(dn1, hat1, scale1, gain_one)
    du = dmid + du
    return du, (gain_grad_one, gain_grad_two), (dq, dk, dv, dp_out, dh, dz)


def weight_grads(kept, cots, out_ref):
    n1, o, n2, g = kept[0], kept[6], kept[7], kept[12]
    dq, dk, dv, dp_out, dh, dz = cots
    lat, lon = out_ref.shape[0], out_ref.shape[1]
    channels = n1.shape[1]
    rows = channels // lat
    g_qkv = jnp.concatenate([mm_tn(n1, part) for part in (dq, dk, dv)], 1)
    g_proj = mm_tn(o, dp_out)
    g_fc1 = mm_tn(n2, dh)
    g_fc2 = mm_tn(g, dz)
    groups = g.shape[1] // channels
    g_fc2 = g_fc2.reshape(lat, groups, rows, channels)
    parts = [g_qkv, g_proj, g_fc1] + [g_fc2[:, a].reshape(channels, channels) for a in range(groups)]
    for j in range(lon):
        pieces = []
        for part in parts:
            width = part.shape[1] // lon
            pieces.append(part[:, j * width : (j + 1) * width])
        mine = jnp.concatenate(pieces, 1).astype(out_ref.dtype)
        for i in range(lat):
            out_ref[i, j] = mine[i * rows : (i + 1) * rows]


def first_kernel(plan, x, cot, to_order, sel_lat, sel_lon, sel_cor, table, row_pick, lane_pick, w_qkv, w_proj, w_fc1, w_fc2, gains,
                 s1, m_lat, m_lon, m_cor, x_ref, bias_ref):
    w = (w_qkv, w_proj, w_fc1, w_fc2)
    expand_bias(0, table, row_pick, lane_pick, x_ref, bias_ref, plan.heads, None)
    u = mm(to_order[...], x[...])
    out, _ = forward(u, 0, gains, w, bias_ref, None, plan)
    both = jnp.concatenate([out, mm(to_order[...], cot[...])], 1).astype(bf16)
    s1[...] = both
    for message, chosen in ((m_lat, sel_lat), (m_lon, sel_lon), (m_cor, sel_cor)):
        message[...] = mm(chosen[...], both).astype(bf16)


def second_kernel(plan, last, s1, r_lat, r_lon, r_cor, roll0, roll1, roll2, roll3, sel_lat, sel_lon, sel_cor,
                  level_mask, late_mask, table, row_pick, lane_pick, w_qkv, w_proj, w_fc1, w_fc2, gains,
                  rolled, m_lat, m_lon, m_cor, grads, gain_out, table_out,
                  x_ref, bias_ref, p_ref, bias_grad_ref, fold_ref):
    w = (w_qkv, w_proj, w_fc1, w_fc2)
    channels = plan.channels
    mask = level_mask[...] + late_mask[...] * last[0].astype(f32)
    expand_bias(1, table, row_pick, lane_pick, x_ref, bias_ref, plan.heads, mask)
    both = mm(roll0[...], s1[...]) + mm(roll1[...], r_lat[...]) + mm(roll2[...], r_lon[...]) + mm(roll3[...], r_cor[...])
    u, cot = both[:, :channels], both[:, channels:]
    _, kept = forward(u, 1, gains, w, bias_ref, p_ref, plan)
    du, gain_grads, cots = backward(cot, kept, 1, gains, w, bias_grad_ref, p_ref, plan)
    du = du.astype(bf16)
    rolled[...] = du
    for message, chosen in ((m_lat, sel_lat), (m_lon, sel_lon), (m_cor, sel_cor)):
        message[...] = mm(chosen[...], du).astype(bf16)
    gain_out[0:1, :] = gain_grads[0]
    gain_out[1:2, :] = gain_grads[1]
    weight_grads(kept, cots, grads)
    fold_bias(bias_grad_ref, row_pick, lane_pick, fold_ref, table_out, plan.heads)


def third_kernel(plan, x, rolled, r_lat, r_lon, r_cor, unroll0, unroll1, unroll2, unroll3, to_order, to_natural,
                 table, row_pick, lane_pick, w_qkv, w_proj, w_fc1, w_fc2, gains,
                 state_grad, grads, gain_out, table_out,
                 x_ref, bias_ref, p_ref, bias_grad_ref, fold_ref):
    w = (w_qkv, w_proj, w_fc1, w_fc2)
    expand_bias(0, table, row_pick, lane_pick, x_ref, bias_ref, plan.heads, None)
    u = mm(to_order[...], x[...])
    _, kept = forward(u, 0, gains, w, bias_ref, p_ref, plan)
    grad = mm(unroll0[...], rolled[...]) + mm(unroll1[...], r_lat[...]) + mm(unroll2[...], r_lon[...]) + mm(unroll3[...], r_cor[...])
    du, gain_grads, cots = backward(grad, kept, 0, gains, w, bias_grad_ref, p_ref, plan)
    state_grad[...] = sum(mm(to_natural[...], part) for part in split3(du))
    gain_out[0:1, :] = gain_grads[0]
    gain_out[1:2, :] = gain_grads[1]
    weight_grads(kept, cots, grads)
    fold_bias(bias_grad_ref, row_pick, lane_pick, fold_ref, table_out, plan.heads)


VMEM_LIMIT = 60 * 1024 * 1024


def call(body, outs, scratch, args, name, flops, scalar=False):
    specs = [pl.BlockSpec(memory_space=pltpu.VMEM) for _ in args]
    if scalar:
        specs[0] = pl.BlockSpec(memory_space=pltpu.SMEM)
    moved = sum(a.size * a.dtype.itemsize for a in args)
    return pl.pallas_call(
        body,
        out_shape=outs,
        in_specs=specs,
        out_specs=[pl.BlockSpec(memory_space=pltpu.VMEM) for _ in outs],
        scratch_shapes=scratch,
        name=name,
        compiler_params=pltpu.CompilerParams(vmem_limit_bytes=VMEM_LIMIT),
        cost_estimate=pl.CostEstimate(flops=flops, bytes_accessed=moved, transcendentals=0),
    )(*args)


def rounded(v):
    return lax.reduce_precision(v, 8, 7)


def body(state, out_cot, qkv_weight, proj_weight, fc1_weight, fc2_weight, norm_gain, bias_table):
    levels, rows, lon, channels = state.shape
    heads = bias_table.shape[3]
    assert levels == WZ and rows == WH and lon % WW == 0
    plan = Plan(lon, heads, channels)
    tokens = plan.tokens
    lats, lons = lax.axis_size("lat"), lax.axis_size("lon")
    count = lats * lons
    axes = ("lat", "lon")
    lat, lon_at = lax.axis_index("lat"), lax.axis_index("lon")
    me = lat * lons + lon_at

    def shift(value, by_lat, by_lon):
        pairs = []
        for a in range(lats):
            for b in range(lons):
                pairs.append((a * lons + b, ((a + by_lat) % lats) * lons + (b + by_lon) % lons))
        return lax.ppermute(value, axes, pairs)

    x = state.reshape(tokens, channels)
    cot = out_cot.reshape(tokens, channels)
    table = bias_table.reshape(2, heads, bias_table.shape[-1])
    weights = (qkv_weight, proj_weight, fc1_weight, fc2_weight)
    n_lat, n_lon, n_cor = plan.sizes
    piece = WH * SPAN
    hidden = fc1_weight.shape[-1]
    columns = sum(a.shape[-1] for a in (qkv_weight, proj_weight, fc1_weight)) // lons + (hidden // channels) * (channels // lons)
    grad_shape = jax.ShapeDtypeStruct((lats, lons, channels // lats, columns), bf16)
    gain_shape = jax.ShapeDtypeStruct((2, channels), f32)
    table_shape = jax.ShapeDtypeStruct((WZ * WZ * WH, heads, piece), f32)
    bias_scratch = [pltpu.VMEM((8 * ZH, 512), f32), pltpu.VMEM((heads, WT, WT), f32)]
    back_scratch = bias_scratch + [
        pltpu.VMEM((plan.windows * heads, WT, WT), f32),
        pltpu.VMEM((heads, WT, WT), f32),
        pltpu.VMEM((16 * heads, 384), f32),
    ]

    def messages(width):
        return [jax.ShapeDtypeStruct((n, width), bf16) for n in plan.sizes]

    flops = 2 * tokens * sum(w.size // 2 for w in weights)
    s1, *out = call(
        functools.partial(first_kernel, plan),
        [jax.ShapeDtypeStruct((tokens, 2 * channels), bf16)] + messages(2 * channels),
        bias_scratch,
        [x, cot, plan.to_order, *plan.send_down, table, plan.row_pick, plan.lane_pick, *weights, norm_gain],
        "first", flops,
    )
    r_lat = shift(out[0], -1, 0)
    r_lon = shift(out[1], 0, -1)
    r_cor = shift(out[2], -1, -1)
    last = (lat == lats - 1).astype(jnp.int32).reshape(1)
    rolled, *out = call(
        functools.partial(second_kernel, plan),
        [jax.ShapeDtypeStruct((tokens, channels), bf16)] + messages(channels) + [grad_shape, gain_shape, table_shape],
        back_scratch,
        [last, s1, r_lat, r_lon, r_cor, *plan.roll, *plan.send_up, plan.level_mask, plan.late_mask,
         table, plan.row_pick, plan.lane_pick, *weights, norm_gain],
        "second", 3 * flops, True,
    )
    r_lat = shift(out[0], 1, 0)
    r_lon = shift(out[1], 0, 1)
    r_cor = shift(out[2], 1, 1)
    grads_two, gain_two, table_two = out[3:]
    state_grad, grads_one, gain_one, table_one = call(
        functools.partial(third_kernel, plan),
        [jax.ShapeDtypeStruct((tokens, channels), f32), grad_shape, gain_shape, table_shape],
        back_scratch,
        [x, rolled, r_lat, r_lon, r_cor, *plan.unroll, plan.to_order, plan.to_natural,
         table, plan.row_pick, plan.lane_pick, *weights, norm_gain],
        "third", 3 * flops,
    )

    bits = count.bit_length() - 1
    lon_bits = lons.bit_length() - 1
    size = grad_shape.shape[2:]
    held = jnp.concatenate((grads_one, grads_two), -1).reshape((2,) * bits + (size[0], 2 * size[1]))
    gain = jnp.concatenate((gain_one, gain_two), 0)
    tables = jnp.stack((table_one, table_two)).transpose(0, 2, 1, 3).reshape(2 * heads, lons, -1)
    tables = tables.transpose(1, 0, 2).reshape((2,) * lon_bits + (2 * heads, -1))
    for bit in range(bits):
        mine = (me >> bit) & 1
        pairs = [(i, i ^ (1 << bit)) for i in range(count)]
        axis = held.ndim - 3
        keep = lax.dynamic_index_in_dim(held, mine, axis, keepdims=False)
        send = lax.dynamic_index_in_dim(held, 1 - mine, axis, keepdims=False)
        high = rounded(gain)
        low = rounded(gain - high)
        extra = jnp.concatenate((high, low), 0).astype(bf16)
        extra = jnp.pad(extra, ((0, 0), (0, 2 * size[1] - channels)))
        message = jnp.concatenate((send.astype(bf16).reshape(-1, 2 * size[1]), extra), 0)
        got = lax.ppermute(message, axes, pairs)
        other = got[-8:, :channels].astype(f32)
        gain = (high + low) + (other[:4] + other[4:])
        held = keep.astype(f32) + got[:-8].reshape(keep.shape).astype(f32)
        if bit < bits - 1:
            held = held.astype(bf16)
        if bit < lon_bits:
            axis = tables.ndim - 3
            keep = lax.dynamic_index_in_dim(tables, mine, axis, keepdims=False)
            send = lax.dynamic_index_in_dim(tables, 1 - mine, axis, keepdims=False)
            tables = keep + lax.ppermute(send.astype(bf16), axes, pairs).astype(f32)

    cuts, start = [], 0
    widths = [w.shape[-1] // lons for w in (qkv_weight, proj_weight, fc1_weight)] + [channels // lons] * (hidden // channels)
    for width in widths:
        cuts.append(jnp.stack((held[:, start : start + width], held[:, size[1] + start : size[1] + start + width])))
        start += width
    fc2 = jnp.concatenate(cuts[3:], 1)
    return (
        state_grad.reshape(state.shape),
        cuts[0],
        cuts[1],
        cuts[2],
        fc2,
        gain.reshape(2, 2, channels),
        tables.reshape(2, 1, 1, heads, -1),
    )


def solution(mesh):
    in_specs = (
        P(None, "lat", "lon", None),
        P(None, "lat", "lon", None),
        P(),
        P(),
        P(),
        P(),
        P(),
        P(None, "lat", None, None, None),
    )
    out_specs = (
        P(None, "lat", "lon", None),
        P(None, "lat", "lon"),
        P(None, "lat", "lon"),
        P(None, "lat", "lon"),
        P(None, "lat", "lon"),
        P(),
        P(None, "lat", None, None, "lon"),
    )
    return jax.shard_map(body, mesh=mesh, in_specs=in_specs, out_specs=out_specs, check_vma=False)
```

```python
import functools

import jax
import jax.numpy as jnp
import numpy as np
from jax import lax
from jax.experimental import pallas as pl
from jax.experimental.pallas import tpu as pltpu
from jax.sharding import PartitionSpec as P

WZ = 2
WH = 6
WW = 12
ZH = WZ * WH
SPAN = 2 * WW - 1
WT = ZH * WW
EPS = 1e-05
NEG = -1e30

f32 = jnp.float32
bf16 = jnp.bfloat16


def one_hot(sources, width):
    table = np.zeros((len(sources), width), np.float32)
    for row, source in enumerate(sources):
        if source >= 0:
            table[row, source] = 1.0
    return jnp.asarray(table, bf16)


class Plan:
    def __init__(self, lon, heads, channels):
        half_h, half_w = WH // 2, WW // 2
        self.lon, self.heads, self.channels = lon, heads, channels
        self.tokens = lon * ZH
        self.windows = lon // WW
        order = [(l, z, h) for l in range(lon) for z in range(WZ) for h in range(WH)]
        self.index = {t: i for i, t in enumerate(order)}
        natural = {(l, z, h): (z * WH + h) * lon + l for l, z, h in order}
        self.to_order = one_hot([natural[t] for t in order], self.tokens)
        place = {natural[t]: i for i, t in enumerate(order)}
        self.to_natural = one_hot([place[i] for i in range(self.tokens)], self.tokens)
        lat_msg = [t for t in order if t[2] < half_h and t[0] >= half_w]
        lon_msg = [t for t in order if t[2] >= half_h and t[0] < half_w]
        cor_msg = [t for t in order if t[2] < half_h and t[0] < half_w]
        self.sizes = (len(lat_msg), len(lon_msg), len(cor_msg))
        self.send_down = [one_hot([self.index[t] for t in m], self.tokens) for m in (lat_msg, lon_msg, cor_msg)]
        picks = ([], [], [], [])
        for l, z, h in order:
            t = (l + half_w, (z + WZ // 2) % WZ, h + half_h)
            over_l, over_h = t[0] >= lon, t[2] >= WH
            t = (t[0] % lon, t[1], t[2] % WH)
            which = {(False, False): 0, (False, True): 1, (True, False): 2, (True, True): 3}[(over_l, over_h)]
            source = self.index[t] if which == 0 else (lat_msg, lon_msg, cor_msg)[which - 1].index(t)
            for i, pick in enumerate(picks):
                pick.append(source if i == which else -1)
        self.roll = [one_hot(picks[0], self.tokens)] + [one_hot(p, n) for p, n in zip(picks[1:], self.sizes)]
        back = {}
        for l, z, h in order:
            t = (l + half_w, (z + WZ // 2) % WZ, h + half_h)
            which = {(False, False): 0, (False, True): 1, (True, False): 2, (True, True): 3}[(t[0] >= lon, t[2] >= WH)]
            back[(t[0] % lon, t[1], t[2] % WH)] = (which, self.index[(l, z, h)])
        msgs = ([], [], [])
        picks = ([], [], [], [])
        for t in order:
            which, source = back[t]
            if which:
                msgs[which - 1].append(source)
            for i, pick in enumerate(picks):
                pick.append((source if which == 0 else len(msgs[which - 1]) - 1) if i == which else -1)
        self.send_up = [one_hot(m, self.tokens) for m in msgs]
        self.unroll = [one_hot(picks[0], self.tokens)] + [one_hot(p, n) for p, n in zip(picks[1:], self.sizes)]
        row = -np.ones(16 * heads, np.int64)
        for h in range(heads):
            for i in range(ZH):
                row[16 * h + i] = 8 * i + h
        self.row_pick = one_hot(row, 8 * ZH)
        lane = -np.ones(384, np.int64)
        for d in range(SPAN):
            for zk in range(WZ):
                for hk in range(WH):
                    lane[(SPAN - 1 - d) * ZH + zk * WH + hk] = zk * 256 + hk * SPAN + d
        self.lane_pick = one_hot(lane, 512).T
        level = np.array([(r % ZH) // WH for r in range(WT)])
        late = np.array([int(r % WH >= WH // 2) for r in range(WT)])
        self.level_mask = jnp.asarray(np.where(level[:, None] == level[None, :], 0.0, NEG), f32)
        self.late_mask = jnp.asarray(np.where(late[:, None] == late[None, :], 0.0, NEG), f32)


def mm(a, b):
    return lax.dot_general(a, b, (((1,), (0,)), ((), ())), preferred_element_type=f32)


def mm_nt(a, b):
    return lax.dot_general(a, b, (((1,), (1,)), ((), ())), preferred_element_type=f32)


def mm_tn(a, b):
    return lax.dot_general(a, b, (((0,), (0,)), ((), ())), preferred_element_type=f32)


def split3(v):
    hi = v.astype(bf16)
    rest = v - hi.astype(f32)
    mid = rest.astype(bf16)
    low = (rest - mid.astype(f32)).astype(bf16)
    return hi, mid, low


def norm(u, gain):
    average = jnp.mean(u, -1, keepdims=True)
    centred = u - average
    scale = lax.rsqrt(jnp.mean(centred * centred, -1, keepdims=True) + EPS)
    hat = centred * scale
    return (hat * gain).astype(bf16), hat, scale


def norm_back(grad, hat, scale, gain):
    inner = grad * gain
    gain_grad = jnp.sum(grad * hat, 0, keepdims=True)
    value = scale * (inner - jnp.mean(inner, -1, keepdims=True) - hat * jnp.mean(inner * hat, -1, keepdims=True))
    return value, gain_grad


def expand_bias(block, table_ref, row_pick, lane_pick, rows_ref, x_ref, bias_ref, heads, mask):
    x_ref[...] = jnp.zeros_like(x_ref)
    for h in range(heads):
        rows_ref[h : h + 1, :] = table_ref[block, h]
    table = rows_ref[0:heads, :]
    piece = WH * SPAN
    for i in range(ZH):
        for zk in range(WZ):
            zq, hq = i // WH, i % WH
            start = ((zq * WZ + zk) * WH + hq) * piece
            x_ref[8 * i : 8 * i + heads, 256 * zk : 256 * zk + piece] = table[:, start : start + piece]
    wide = None
    for part in split3(x_ref[...]):
        moved = mm(mm(row_pick[...], part).astype(bf16), lane_pick[...])
        wide = moved if wide is None else wide + moved
    for w in range(WW):
        start = (WW - 1 - w) * ZH
        turned = pltpu.roll(wide, (384 - start) % 384, 1) if start else wide
        for h in range(heads):
            rows = turned[16 * h : 16 * h + ZH, 0:WT]
            if mask is not None:
                rows = rows + mask[ZH * w : ZH * w + ZH, :]
            bias_ref[h, ZH * w : ZH * w + ZH, :] = rows


def fold_bias(bias_grad_ref, row_pick, lane_pick, fold_ref, out_ref, heads):
    fold_ref[...] = jnp.zeros_like(fold_ref)
    total = None
    for w in range(WW):
        for h in range(heads):
            fold_ref[16 * h : 16 * h + ZH, 0:WT] = bias_grad_ref[h, ZH * w : ZH * w + ZH, :]
        start = (WW - 1 - w) * ZH
        turned = fold_ref[...]
        if start:
            turned = pltpu.roll(turned, start, 1)
        total = turned if total is None else total + turned
    back = mm_nt(mm_tn(row_pick[...], total.astype(bf16)).astype(bf16), lane_pick[...])
    piece = WH * SPAN
    chunk = out_ref.shape[2]
    for i in range(ZH):
        for zk in range(WZ):
            zq, hq = i // WH, i % WH
            start = ((zq * WZ + zk) * WH + hq) * piece
            at = start
            while at < start + piece:
                j = at // chunk
                end = min(start + piece, (j + 1) * chunk)
                lane = 256 * zk + at - start
                out_ref[j, :, at - j * chunk : end - j * chunk] = back[8 * i : 8 * i + heads, lane : lane + end - at]
                at = end


def head_masks(heads, channels):
    lanes = lax.broadcasted_iota(jnp.int32, (1, channels), 1)
    size = channels // heads
    return [(lanes >= size * h) & (lanes < size * (h + 1)) for h in range(heads)]


def pick(mask, value):
    return jnp.where(mask, value, jnp.zeros_like(value))


def forward(u, block, gains, w, bias_ref, p_ref, plan, outs=None):
    channels, heads = plan.channels, plan.heads
    w_qkv, w_proj, w_fc1, w_fc2 = w
    n1, hat1, scale1 = norm(u, gains[block, 0:1, :])
    qkv_w = w_qkv[block]
    q, k, v = (mm(n1, qkv_w[:, i * channels : (i + 1) * channels]).astype(bf16) for i in range(3))
    masks = head_masks(heads, channels)
    factor = (channels // heads) ** (-0.5)
    joined = []
    for n in range(plan.windows):
        rows = slice(n * WT, (n + 1) * WT)
        qw, kw, vw = q[rows], k[rows], v[rows]
        total = None
        for h in range(heads):
            s = mm_nt(pick(masks[h], qw), kw) * factor + bias_ref[h]
            e = jnp.exp(s - jnp.max(s, -1, keepdims=True))
            p = e / jnp.sum(e, -1, keepdims=True)
            p_ref[n * heads + h] = p
            o = mm(p.astype(bf16), pick(masks[h], vw))
            total = o if total is None else total + o
        joined.append(total.astype(bf16))
    o = jnp.concatenate(joined, 0)
    middle = u + mm(o, w_proj[block])
    n2, hat2, scale2 = norm(middle, gains[block, 1:2, :])
    wide = mm(n2, w_fc1[block])
    cdf = 0.5 * (1.0 + lax.erf(wide * (0.5**0.5)))
    g = (wide * cdf).astype(bf16)
    return (n1, hat1, scale1, q, k, v, o, middle, n2, hat2, scale2, wide, cdf, g)


def slope(wide, cdf):
    return cdf + wide * (jnp.exp(-0.5 * wide * wide) * (1.0 / np.sqrt(2.0 * np.pi)))


def mlp_back(grad, block, gains, w, hat2, scale2, gelu_slope):
    _, _, w_fc1, w_fc2 = w
    dz = grad.astype(bf16)
    dg = mm(dz, w_fc2[block]).astype(bf16).astype(f32)
    dh = (dg * gelu_slope).astype(bf16)
    dn2 = mm_nt(dh, w_fc1[block]).astype(bf16).astype(f32)
    dmid, gain_grad = norm_back(dn2, hat2, scale2, gains[block, 1:2, :])
    return grad + dmid, gain_grad, dz, dh


def attention_back(dmid, block, gains, w, n1, hat1, scale1, q, k, v, p_ref, bias_grad_ref, plan):
    channels, heads = plan.channels, plan.heads
    w_qkv, w_proj, _, _ = w
    dp_out = dmid.astype(bf16)
    do = mm_nt(dp_out, w_proj[block]).astype(bf16)
    masks = head_masks(heads, channels)
    factor = (channels // heads) ** (-0.5)
    dqs, dks, dvs = [], [], []
    for n in range(plan.windows):
        rows = slice(n * WT, (n + 1) * WT)
        qw, kw, vw, dow = q[rows], k[rows], v[rows], do[rows]
        dq = dk = dv = None
        for h in range(heads):
            dom = pick(masks[h], dow)
            p = p_ref[n * heads + h]
            dp = mm_nt(dom, vw).astype(bf16).astype(f32)
            ds = p * (dp - jnp.sum(dp * p, -1, keepdims=True))
            if n == 0:
                bias_grad_ref[h] = ds
            else:
                bias_grad_ref[h] += ds
            dsb = (ds * factor).astype(bf16)
            a = mm(dsb, pick(masks[h], kw))
            b = mm_tn(dsb, pick(masks[h], qw))
            c = mm_tn(p.astype(bf16), dom)
            dq, dk, dv = (a, b, c) if dq is None else (dq + a, dk + b, dv + c)
        dqs.append(dq.astype(bf16))
        dks.append(dk.astype(bf16))
        dvs.append(dv.astype(bf16))
    dq, dk, dv = (jnp.concatenate(parts, 0) for parts in (dqs, dks, dvs))
    qkv_w = w_qkv[block]
    dn1 = None
    for i, part in enumerate((dq, dk, dv)):
        term = mm_nt(part, qkv_w[:, i * channels : (i + 1) * channels])
        dn1 = term if dn1 is None else dn1 + term
    dn1 = dn1.astype(bf16).astype(f32)
    du, gain_grad = norm_back(dn1, hat1, scale1, gains[block, 0:1, :])
    return dmid + du, gain_grad, dq, dk, dv, dp_out


def put_slices(parts, out_ref):
    lat, lon, rows = out_ref.shape[:3]
    for j in range(lon):
        pieces = []
        for part in parts:
            width = part.shape[1] // lon
            pieces.append(part[:, j * width : (j + 1) * width])
        mine = jnp.concatenate(pieces, 1).astype(out_ref.dtype)
        for i in range(lat):
            out_ref[i, j] = mine[i * rows : (i + 1) * rows]


def attention_weights(n1, o, dq, dk, dv, dp_out):
    return [jnp.concatenate([mm_tn(n1, part) for part in (dq, dk, dv)], 1), mm_tn(o, dp_out)]


def mlp_weights(n2, g, dh, dz, lat):
    channels = n2.shape[1]
    groups = g.shape[1] // channels
    g_fc2 = mm_tn(g, dz).reshape(lat, groups, channels // lat, channels)
    return [mm_tn(n2, dh)] + [g_fc2[:, a].reshape(channels, channels) for a in range(groups)]


KEPT = ("n1", "hat1", "scale1", "q", "k", "v", "o", "n2", "hat2", "scale2", "wide", "cdf", "g")


def first_kernel(plan, x, cot, to_order, sel_lat, sel_lon, sel_cor, table, row_pick, lane_pick, w_qkv, w_proj, w_fc1, w_fc2, gains,
                 s1, m_lat, m_lon, m_cor, p_out, *rest):
    kept_refs, (rows_ref, x_ref, bias_ref) = rest[:-3], rest[-3:]
    w = (w_qkv, w_proj, w_fc1, w_fc2)
    expand_bias(0, table, row_pick, lane_pick, rows_ref, x_ref, bias_ref, plan.heads, None)
    u = mm(to_order[...], x[...])
    kept = forward(u, 0, gains, w, bias_ref, p_out, plan)
    middle, g = kept[7], kept[13]
    out = middle + mm_nt(g, w_fc2[0])
    both = jnp.concatenate([out, mm(to_order[...], cot[...])], 1).astype(bf16)
    s1[...] = both
    for message, chosen in ((m_lat, sel_lat), (m_lon, sel_lon), (m_cor, sel_cor)):
        message[...] = mm(chosen[...], both).astype(bf16)
    for ref, value in zip(kept_refs, kept[:7] + kept[8:]):
        ref[...] = value


def between_kernel(plan, last, level_mask, late_mask, table, row_pick, lane_pick, wide, cdf, bias_out, slope_out, rows_ref, x_ref):
    mask = level_mask[...] + late_mask[...] * last[0].astype(f32)
    expand_bias(1, table, row_pick, lane_pick, rows_ref, x_ref, bias_out, plan.heads, mask)
    slope_out[...] = slope(wide[...], cdf[...])


def second_kernel(plan, s1, r_lat, r_lon, r_cor, roll0, roll1, roll2, roll3, sel_lat, sel_lon, sel_cor,
                  bias_ref, w_qkv, w_proj, w_fc1, w_fc2, gains,
                  rolled, m_lat, m_lon, m_cor, gain_out, bias_grad_ref,
                  n1_out, o_out, n2_out, g_out, dq_out, dk_out, dv_out, dp_out_out, dh_out, dz_out, p_ref):
    w = (w_qkv, w_proj, w_fc1, w_fc2)
    channels = plan.channels
    both = mm(roll0[...], s1[...]) + mm(roll1[...], r_lat[...]) + mm(roll2[...], r_lon[...]) + mm(roll3[...], r_cor[...])
    u, cot = both[:, :channels], both[:, channels:]
    n1, hat1, scale1, q, k, v, o, middle, n2, hat2, scale2, wide, cdf, g = forward(u, 1, gains, w, bias_ref, p_ref, plan)
    dmid, gain_two, dz, dh = mlp_back(cot, 1, gains, w, hat2, scale2, slope(wide, cdf))
    du, gain_one, dq, dk, dv, dp_out = attention_back(dmid, 1, gains, w, n1, hat1, scale1, q, k, v, p_ref, bias_grad_ref, plan)
    du = du.astype(bf16)
    rolled[...] = du
    for message, chosen in ((m_lat, sel_lat), (m_lon, sel_lon), (m_cor, sel_cor)):
        message[...] = mm(chosen[...], du).astype(bf16)
    gain_out[0:1, :] = gain_one
    gain_out[1:2, :] = gain_two
    for ref, value in ((n1_out, n1), (o_out, o), (n2_out, n2), (g_out, g), (dq_out, dq), (dk_out, dk), (dv_out, dv),
                       (dp_out_out, dp_out), (dh_out, dh), (dz_out, dz)):
        ref[...] = value


def grads_kernel(plan, n1, o, n2, g, dq, dk, dv, dp_out, dh, dz, bias_grad_ref, row_pick, lane_pick, grads, table_out, fold_ref):
    parts = attention_weights(n1[...], o[...], dq[...], dk[...], dv[...], dp_out[...])
    parts += mlp_weights(n2[...], g[...], dh[...], dz[...], grads.shape[0])
    put_slices(parts, grads)
    fold_bias(bias_grad_ref, row_pick, lane_pick, fold_ref, table_out, plan.heads)


def third_kernel(plan, rolled, r_lat, r_lon, r_cor, unroll0, unroll1, unroll2, unroll3,
                 n2, hat2, scale2, gelu_slope, g, w_fc1, w_fc2, gains,
                 dmid_out, gain_out, grads):
    grad = mm(unroll0[...], rolled[...]) + mm(unroll1[...], r_lat[...]) + mm(unroll2[...], r_lon[...]) + mm(unroll3[...], r_cor[...])
    dmid, gain_two, dz, dh = mlp_back(grad, 0, gains, (None, None, w_fc1, w_fc2), hat2[...], scale2[...], gelu_slope[...])
    dmid_out[...] = dmid
    gain_out[...] = gain_two
    put_slices(mlp_weights(n2[...], g[...], dh, dz, grads.shape[0]), grads)


def fourth_kernel(plan, dmid, n1, hat1, scale1, q, k, v, o, p_ref, w_qkv, w_proj, gains, to_natural, row_pick, lane_pick,
                  state_grad, gain_out, grads, table_out, bias_grad_ref, fold_ref):
    n1 = n1[...]
    du, gain_one, dq, dk, dv, dp_out = attention_back(
        dmid[...], 0, gains, (w_qkv, w_proj, None, None), n1, hat1[...], scale1[...], q[...], k[...], v[...], p_ref, bias_grad_ref, plan)
    put_slices(attention_weights(n1, o[...], dq, dk, dv, dp_out), grads)
    gain_out[...] = gain_one
    fold_bias(bias_grad_ref, row_pick, lane_pick, fold_ref, table_out, plan.heads)
    state_grad[...] = sum(mm(to_natural[...], part) for part in split3(du))


def last_kernel(widths, one_a, one_b, two, qkv, proj, fc1, fc2):
    w_qkv, w_proj, w_fc1, w_fc2 = widths
    for b, (attention, mlp) in enumerate(((one_a[...], one_b[...]), (two[:, : w_qkv + w_proj], two[:, w_qkv + w_proj :]))):
        qkv[b] = attention[:, :w_qkv]
        proj[b] = attention[:, w_qkv:]
        fc1[b] = mlp[:, :w_fc1]
        groups = (mlp.shape[1] - w_fc1) // w_fc2
        tall = jnp.concatenate([mlp[:, w_fc1 + w_fc2 * a : w_fc1 + w_fc2 * (a + 1)] for a in range(groups)], 0)
        fc2[b] = tall.T


def call(body, outs, scratch, args, name, flops, limit, scalar=False):
    specs = [pl.BlockSpec(memory_space=pltpu.VMEM) for _ in args]
    if scalar:
        specs[0] = pl.BlockSpec(memory_space=pltpu.SMEM)
    moved = sum(a.size * a.dtype.itemsize for a in args)
    return pl.pallas_call(
        body,
        out_shape=outs,
        in_specs=specs,
        out_specs=[pl.BlockSpec(memory_space=pltpu.VMEM) for _ in outs],
        scratch_shapes=scratch,
        name=name,
        compiler_params=pltpu.CompilerParams(vmem_limit_bytes=limit * 1024 * 1024),
        cost_estimate=pl.CostEstimate(flops=flops, bytes_accessed=moved, transcendentals=0),
    )(*args)


def rounded(v):
    return lax.reduce_precision(v, 8, 7)


def body(state, out_cot, qkv_weight, proj_weight, fc1_weight, fc2_weight, norm_gain, bias_table):
    levels, rows, lon, channels = state.shape
    heads = bias_table.shape[3]
    assert levels == WZ and rows == WH and lon % WW == 0
    plan = Plan(lon, heads, channels)
    tokens, windows = plan.tokens, plan.windows
    lats, lons = lax.axis_size("lat"), lax.axis_size("lon")
    count = lats * lons
    axes = ("lat", "lon")
    lat, lon_at = lax.axis_index("lat"), lax.axis_index("lon")
    me = lat * lons + lon_at

    def shift(value, by_lat, by_lon):
        pairs = []
        for a in range(lats):
            for b in range(lons):
                pairs.append((a * lons + b, ((a + by_lat) % lats) * lons + (b + by_lon) % lons))
        return lax.ppermute(value, axes, pairs)

    def shape(*dims, kind=bf16):
        return jax.ShapeDtypeStruct(dims, kind)

    x = state.reshape(tokens, channels)
    cot = out_cot.reshape(tokens, channels)
    entries = bias_table.shape[-1]
    table = bias_table.reshape(2, heads, 1, entries)
    w_qkv, w_proj, w_fc1 = qkv_weight, proj_weight, fc1_weight
    w_fc2 = fc2_weight.transpose(0, 2, 1)
    weights = (w_qkv, w_proj, w_fc1, w_fc2)
    hidden = fc1_weight.shape[-1]
    groups = hidden // channels
    widths = tuple(w.shape[-1] // lons for w in (w_qkv, w_proj, w_fc1)) + (channels // lons,)
    part_a = widths[0] + widths[1]
    part_b = widths[2] + groups * widths[3]
    slice_rows = channels // lats
    table_shape = shape(lons, heads, entries // lons, kind=f32)
    bias_shape = shape(heads, WT, WT, kind=f32)
    expand_scratch = [pltpu.VMEM((8, entries), f32), pltpu.VMEM((8 * ZH, 512), f32)]
    bias_scratch = pltpu.VMEM((heads, WT, WT), f32)
    fold_scratch = pltpu.VMEM((16 * heads, 384), f32)
    wide_f32 = shape(tokens, channels, kind=f32)
    narrow = shape(tokens, channels)
    column = shape(tokens, 1, kind=f32)

    def messages(width):
        return [shape(n, width) for n in plan.sizes]

    flops = 2 * tokens * sum(w.size // 2 for w in weights)
    kept_shapes = [narrow, wide_f32, column, narrow, narrow, narrow, narrow, narrow, wide_f32, column,
                   shape(tokens, hidden, kind=f32), shape(tokens, hidden, kind=f32), shape(tokens, hidden)]
    s1, m_lat, m_lon, m_cor, p_one, *kept = call(
        functools.partial(first_kernel, plan),
        [shape(tokens, 2 * channels)] + messages(2 * channels) + [shape(windows * heads, WT, WT, kind=f32)] + kept_shapes,
        expand_scratch + [bias_scratch],
        [x, cot, plan.to_order, *plan.send_down, table, plan.row_pick, plan.lane_pick, *weights, norm_gain],
        "first", flops, FIRST,
    )
    kept = dict(zip(KEPT, kept))
    r_lat = shift(m_lat, -1, 0)
    r_lon = shift(m_lon, 0, -1)
    r_cor = shift(m_cor, -1, -1)
    last = (lat == lats - 1).astype(jnp.int32).reshape(1)
    bias_two, gelu_slope = call(
        functools.partial(between_kernel, plan),
        [bias_shape, shape(tokens, hidden, kind=f32)],
        expand_scratch,
        [last, plan.level_mask, plan.late_mask, table, plan.row_pick, plan.lane_pick, kept["wide"], kept["cdf"]],
        "between", flops, BETWEEN, True,
    )
    rolled, m_lat, m_lon, m_cor, gain_two, bias_grad, *saved = call(
        functools.partial(second_kernel, plan),
        [narrow] + messages(channels) + [shape(2, channels, kind=f32), bias_shape]
        + [narrow, narrow, narrow, shape(tokens, hidden), narrow, narrow, narrow, narrow, shape(tokens, hidden), narrow],
        [pltpu.VMEM((windows * heads, WT, WT), f32)],
        [s1, r_lat, r_lon, r_cor, *plan.roll, *plan.send_up, bias_two, *weights, norm_gain],
        "second", 2 * flops, SECOND,
    )
    r_lat = shift(m_lat, 1, 0)
    r_lon = shift(m_lon, 0, 1)
    r_cor = shift(m_cor, 1, 1)
    grads_two, table_two = call(
        functools.partial(grads_kernel, plan),
        [shape(lats, lons, slice_rows, part_a + part_b), table_shape],
        [fold_scratch],
        [*saved, bias_grad, plan.row_pick, plan.lane_pick],
        "grads", flops, GRADS,
    )
    dmid, gain_one_b, grads_one_b = call(
        functools.partial(third_kernel, plan),
        [wide_f32, shape(1, channels, kind=f32), shape(lats, lons, slice_rows, part_b)],
        [],
        [rolled, r_lat, r_lon, r_cor, *plan.unroll, kept["n2"], kept["hat2"], kept["scale2"], gelu_slope, kept["g"],
         w_fc1, w_fc2, norm_gain],
        "third", flops, THIRD,
    )
    state_grad, gain_one_a, grads_one_a, table_one = call(
        functools.partial(fourth_kernel, plan),
        [wide_f32, shape(1, channels, kind=f32), shape(lats, lons, slice_rows, part_a), table_shape],
        [bias_scratch, fold_scratch],
        [dmid, kept["n1"], kept["hat1"], kept["scale1"], kept["q"], kept["k"], kept["v"], kept["o"], p_one,
         w_qkv, w_proj, norm_gain, plan.to_natural, plan.row_pick, plan.lane_pick],
        "fourth", flops, FOURTH,
    )

    bits = count.bit_length() - 1
    lon_bits = lons.bit_length() - 1

    def exchange(value, bit):
        return lax.ppermute(value, axes, [(i, i ^ (1 << bit)) for i in range(count)])

    def halves(held, bit):
        mine = (me >> bit) & 1
        axis = held.ndim - 3
        keep = lax.dynamic_index_in_dim(held, mine, axis, keepdims=False)
        send = lax.dynamic_index_in_dim(held, 1 - mine, axis, keepdims=False)
        return keep.astype(f32), send.astype(bf16)

    def scatter(value, first, stop, whole):
        for bit in range(first, stop):
            keep, send = halves(value, bit)
            value = keep + exchange(send, bit).astype(f32)
            if bit < whole - 1:
                value = value.astype(bf16)
        return value

    def split(value, how_many):
        return value.reshape((2,) * how_many + value.shape[-2:])

    gain = jnp.concatenate((gain_one_a, gain_one_b, gain_two), 0)
    two = scatter(split(grads_two, bits), 0, bits, bits)
    one_b = scatter(split(grads_one_b, bits), 0, 1, bits)
    one_a = split(grads_one_a, bits)
    tables = [scatter(split(t, lon_bits), 0, lon_bits, lon_bits) for t in (table_one, table_two)]
    for bit in range(bits):
        keep, send = halves(one_a, bit)
        high = rounded(gain)
        low = rounded(gain - high)
        extra = jnp.concatenate((high, low), 0).astype(bf16)
        flat = jnp.pad(extra.reshape(-1), (0, -extra.size % part_a)).reshape(-1, part_a)
        got = exchange(jnp.concatenate((send.reshape(-1, part_a), flat), 0), bit)
        other = got[-flat.shape[0] :].reshape(-1)[: extra.size].reshape(extra.shape).astype(f32)
        gain = (high + low) + (other[:4] + other[4:])
        one_a = keep + got[: -flat.shape[0]].reshape(keep.shape).astype(f32)
        if bit < bits - 1:
            one_a = one_a.astype(bf16)
    one_b = scatter(one_b, 1, bits, bits)
    qkv, proj, fc1, fc2 = call(
        functools.partial(last_kernel, widths),
        [shape(2, slice_rows, n, kind=f32) for n in widths[:3]] + [shape(2, widths[3], groups * slice_rows, kind=f32)],
        [], [one_a, one_b, two], "last", 1000, 4,
    )
    return (
        state_grad.reshape(state.shape),
        qkv,
        proj,
        fc1,
        fc2.transpose(0, 2, 1),
        gain.reshape(2, 2, channels),
        jnp.stack(tables).reshape(2, 1, 1, heads, -1),
    )


FIRST, BETWEEN, SECOND, GRADS, THIRD, FOURTH = 8, 8, 8, 8, 8, 8


def solution(mesh):
    in_specs = (
        P(None, "lat", "lon", None),
        P(None, "lat", "lon", None),
        P(),
        P(),
        P(),
        P(),
        P(),
        P(None, "lat", None, None, None),
    )
    out_specs = (
        P(None, "lat", "lon", None),
        P(None, "lat", "lon"),
        P(None, "lat", "lon"),
        P(None, "lat", "lon"),
        P(None, "lat", "lon"),
        P(),
        P(None, "lat", None, None, "lon"),
    )
    return jax.shard_map(body, mesh=mesh, in_specs=in_specs, out_specs=out_specs, check_vma=False)
```

```python
import functools

import jax
import jax.numpy as jnp
import numpy as np
from jax import lax
from jax.experimental import pallas as pl
from jax.experimental.pallas import tpu as pltpu
from jax.sharding import PartitionSpec as P

WZ = 2
WH = 6
WW = 12
ZH = WZ * WH
SPAN = 2 * WW - 1
WT = ZH * WW
EPS = 1e-05
NEG = -1e30

f32 = jnp.float32
bf16 = jnp.bfloat16


def one_hot(sources, width):
    table = np.zeros((len(sources), width), np.float32)
    for row, source in enumerate(sources):
        if source >= 0:
            table[row, source] = 1.0
    return jnp.asarray(table, bf16)


class Plan:
    def __init__(self, lon, heads, channels):
        half_h, half_w = WH // 2, WW // 2
        self.lon, self.heads, self.channels = lon, heads, channels
        self.tokens = lon * ZH
        self.windows = lon // WW
        order = [(l, z, h) for l in range(lon) for z in range(WZ) for h in range(WH)]
        self.index = {t: i for i, t in enumerate(order)}
        natural = {(l, z, h): (z * WH + h) * lon + l for l, z, h in order}
        self.to_order = one_hot([natural[t] for t in order], self.tokens)
        place = {natural[t]: i for i, t in enumerate(order)}
        self.to_natural = one_hot([place[i] for i in range(self.tokens)], self.tokens)
        lat_msg = [t for t in order if t[2] < half_h and t[0] >= half_w]
        lon_msg = [t for t in order if t[2] >= half_h and t[0] < half_w]
        cor_msg = [t for t in order if t[2] < half_h and t[0] < half_w]
        self.sizes = (len(lat_msg), len(lon_msg), len(cor_msg))
        self.send_down = [one_hot([self.index[t] for t in m], self.tokens) for m in (lat_msg, lon_msg, cor_msg)]
        picks = ([], [], [], [])
        for l, z, h in order:
            t = (l + half_w, (z + WZ // 2) % WZ, h + half_h)
            over_l, over_h = t[0] >= lon, t[2] >= WH
            t = (t[0] % lon, t[1], t[2] % WH)
            which = {(False, False): 0, (False, True): 1, (True, False): 2, (True, True): 3}[(over_l, over_h)]
            source = self.index[t] if which == 0 else (lat_msg, lon_msg, cor_msg)[which - 1].index(t)
            for i, pick in enumerate(picks):
                pick.append(source if i == which else -1)
        self.roll = [one_hot(picks[0], self.tokens)] + [one_hot(p, n) for p, n in zip(picks[1:], self.sizes)]
        back = {}
        for l, z, h in order:
            t = (l + half_w, (z + WZ // 2) % WZ, h + half_h)
            which = {(False, False): 0, (False, True): 1, (True, False): 2, (True, True): 3}[(t[0] >= lon, t[2] >= WH)]
            back[(t[0] % lon, t[1], t[2] % WH)] = (which, self.index[(l, z, h)])
        msgs = ([], [], [])
        picks = ([], [], [], [])
        for t in order:
            which, source = back[t]
            if which:
                msgs[which - 1].append(source)
            for i, pick in enumerate(picks):
                pick.append((source if which == 0 else len(msgs[which - 1]) - 1) if i == which else -1)
        self.send_up = [one_hot(m, self.tokens) for m in msgs]
        self.unroll = [one_hot(picks[0], self.tokens)] + [one_hot(p, n) for p, n in zip(picks[1:], self.sizes)]
        row = -np.ones(16 * heads, np.int64)
        for h in range(heads):
            for i in range(ZH):
                row[16 * h + i] = 8 * i + h
        self.row_pick = one_hot(row, 8 * ZH)
        lane = -np.ones(384, np.int64)
        for d in range(SPAN):
            for zk in range(WZ):
                for hk in range(WH):
                    lane[(SPAN - 1 - d) * ZH + zk * WH + hk] = zk * 256 + hk * SPAN + d
        self.lane_pick = one_hot(lane, 512).T
        level = np.array([(r % ZH) // WH for r in range(WT)])
        late = np.array([int(r % WH >= WH // 2) for r in range(WT)])
        self.level_mask = jnp.asarray(np.where(level[:, None] == level[None, :], 0.0, NEG), f32)
        self.late_mask = jnp.asarray(np.where(late[:, None] == late[None, :], 0.0, NEG), f32)


def mm(a, b):
    return lax.dot_general(a, b, (((1,), (0,)), ((), ())), preferred_element_type=f32)


def mm_nt(a, b):
    return lax.dot_general(a, b, (((1,), (1,)), ((), ())), preferred_element_type=f32)


def mm_tn(a, b):
    return lax.dot_general(a, b, (((0,), (0,)), ((), ())), preferred_element_type=f32)


def split3(v):
    hi = v.astype(bf16)
    rest = v - hi.astype(f32)
    mid = rest.astype(bf16)
    low = (rest - mid.astype(f32)).astype(bf16)
    return hi, mid, low


def norm(u, gain):
    average = jnp.mean(u, -1, keepdims=True)
    centred = u - average
    scale = lax.rsqrt(jnp.mean(centred * centred, -1, keepdims=True) + EPS)
    hat = centred * scale
    return (hat * gain).astype(bf16), hat, scale


def norm_back(grad, hat, scale, gain):
    inner = grad * gain
    gain_grad = jnp.sum(grad * hat, 0, keepdims=True)
    value = scale * (inner - jnp.mean(inner, -1, keepdims=True) - hat * jnp.mean(inner * hat, -1, keepdims=True))
    return value, gain_grad


def expand_bias(table_ref, row_pick, lane_pick, rows_ref, x_ref, bias_ref, heads, mask):
    x_ref[...] = jnp.zeros_like(x_ref)
    for h in range(heads):
        rows_ref[h : h + 1, :] = table_ref[h]
    table = rows_ref[0:heads, :]
    piece = WH * SPAN
    for i in range(ZH):
        for zk in range(WZ):
            zq, hq = i // WH, i % WH
            start = ((zq * WZ + zk) * WH + hq) * piece
            x_ref[8 * i : 8 * i + heads, 256 * zk : 256 * zk + piece] = table[:, start : start + piece]
    wide = None
    for part in split3(x_ref[...]):
        moved = mm(mm(row_pick[...], part).astype(bf16), lane_pick[...])
        wide = moved if wide is None else wide + moved
    for w in range(WW):
        start = (WW - 1 - w) * ZH
        turned = pltpu.roll(wide, (384 - start) % 384, 1) if start else wide
        for h in range(heads):
            rows = turned[16 * h : 16 * h + ZH, 0:WT]
            if mask is not None:
                rows = rows + mask[ZH * w : ZH * w + ZH, :]
            bias_ref[h, ZH * w : ZH * w + ZH, :] = rows


class Board:
    def __init__(self, lats, lons, channels, width, entries):
        self.lats, self.lons, self.channels, self.width = lats, lons, channels, width
        self.rows = channels // lats
        self.half = lons // 2
        self.chunk = entries // lons
        self.segments = -(-self.chunk // width)
        self.gain_segments = -(-channels // width)
        self.table_at = lats * self.half * self.rows
        self.gain_at = self.table_at + self.half * 8 * self.segments
        self.total = self.gain_at + 8

    def put_slices(self, ref, side, parts):
        for j in range(self.lons):
            pieces = []
            for part in parts:
                wide = part.shape[1] // self.lons
                pieces.append(part[:, j * wide : (j + 1) * wide])
            mine = jnp.concatenate(pieces, 1)
            at = side[j % 2]
            for i in range(self.lats):
                row = (i * self.half + j // 2) * self.rows
                ref[at, row : row + self.rows, :] = mine[i * self.rows : (i + 1) * self.rows]

    def put_table(self, ref, side, back, heads):
        piece = WH * SPAN
        for i in range(ZH):
            for zk in range(WZ):
                zq, hq = i // WH, i % WH
                start = ((zq * WZ + zk) * WH + hq) * piece
                at = start
                while at < start + piece:
                    j, inside = at // self.chunk, at % self.chunk
                    segment = inside // self.width
                    end = min(start + piece, (j + 1) * self.chunk, j * self.chunk + (segment + 1) * self.width)
                    lane = 256 * zk + at - start
                    row = self.table_at + ((j // 2) * self.segments + segment) * 8
                    first = inside - segment * self.width
                    value = back[8 * i : 8 * i + heads, lane : lane + end - at]
                    ref[side[j % 2], row : row + heads, first : first + end - at] = value
                    at = end

    def put_gains(self, ref, gains):
        both = []
        for part in range(2):
            for gain in gains:
                high = gain.astype(bf16).astype(f32)
                both.append(high if part == 0 else gain - high)
        for n, value in enumerate(both):
            for segment in range(self.gain_segments):
                cut = value[:, segment * self.width : min(self.channels, (segment + 1) * self.width)]
                row = self.gain_at + n * self.gain_segments + segment
                for at in range(2):
                    ref[at, row : row + 1, 0 : cut.shape[1]] = cut


def fold_bias(bias_grad_ref, row_pick, lane_pick, fold_ref, heads):
    fold_ref[...] = jnp.zeros_like(fold_ref)
    total = None
    for w in range(WW):
        for h in range(heads):
            fold_ref[16 * h : 16 * h + ZH, 0:WT] = bias_grad_ref[h, ZH * w : ZH * w + ZH, :]
        start = (WW - 1 - w) * ZH
        turned = fold_ref[...]
        if start:
            turned = pltpu.roll(turned, start, 1)
        total = turned if total is None else total + turned
    return mm_nt(mm_tn(row_pick[...], total.astype(bf16)).astype(bf16), lane_pick[...])


def head_masks(heads, channels):
    lanes = lax.broadcasted_iota(jnp.int32, (1, channels), 1)
    size = channels // heads
    return [(lanes >= size * h) & (lanes < size * (h + 1)) for h in range(heads)]


def pick(mask, value):
    return jnp.where(mask, value, jnp.zeros_like(value))


def forward(u, gains, w, bias_ref, p_ref, plan):
    channels, heads = plan.channels, plan.heads
    w_qkv, w_proj, w_fc1 = w
    n1, hat1, scale1 = norm(u, gains[0:1, :])
    qkv_w = w_qkv[...]
    q, k, v = (mm(n1, qkv_w[:, i * channels : (i + 1) * channels]).astype(bf16) for i in range(3))
    masks = head_masks(heads, channels)
    factor = (channels // heads) ** (-0.5)
    joined = []
    for n in range(plan.windows):
        rows = slice(n * WT, (n + 1) * WT)
        qw, kw, vw = q[rows], k[rows], v[rows]
        total = None
        for h in range(heads):
            s = mm_nt(pick(masks[h], qw), kw) * factor + bias_ref[h]
            e = jnp.exp(s - jnp.max(s, -1, keepdims=True))
            p = e / jnp.sum(e, -1, keepdims=True)
            p_ref[n * heads + h] = p.astype(p_ref.dtype)
            o = mm(p.astype(bf16), pick(masks[h], vw))
            total = o if total is None else total + o
        joined.append(total.astype(bf16))
    o = jnp.concatenate(joined, 0)
    middle = u + mm(o, w_proj[...])
    n2, hat2, scale2 = norm(middle, gains[1:2, :])
    wide = mm(n2, w_fc1[...])
    cdf = 0.5 * (1.0 + lax.erf(wide * (0.5**0.5)))
    g = (wide * cdf).astype(bf16)
    return (n1, hat1, scale1, q, k, v, o, middle, n2, hat2, scale2, wide, cdf, g)


def slope(wide, cdf):
    return cdf + wide * (jnp.exp(-0.5 * wide * wide) * (1.0 / np.sqrt(2.0 * np.pi)))


def mlp_back(grad, gains, w, hat2, scale2, gelu_slope):
    w_fc1, w_fc2 = w
    dz = grad.astype(bf16)
    dg = mm(dz, w_fc2[...]).astype(bf16).astype(f32)
    dh = (dg * gelu_slope).astype(bf16)
    dn2 = mm_nt(dh, w_fc1[...]).astype(bf16).astype(f32)
    dmid, gain_grad = norm_back(dn2, hat2, scale2, gains[1:2, :])
    return grad + dmid, gain_grad, dz, dh


def attention_back(dmid, gains, w, hat1, scale1, q, k, v, p_ref, bias_grad_ref, plan):
    channels, heads = plan.channels, plan.heads
    w_qkv, w_proj = w
    dp_out = dmid.astype(bf16)
    do = mm_nt(dp_out, w_proj[...]).astype(bf16)
    masks = head_masks(heads, channels)
    factor = (channels // heads) ** (-0.5)
    dqs, dks, dvs = [], [], []
    for n in range(plan.windows):
        rows = slice(n * WT, (n + 1) * WT)
        qw, kw, vw, dow = q[rows], k[rows], v[rows], do[rows]
        dq = dk = dv = None
        for h in range(heads):
            dom = pick(masks[h], dow)
            p = p_ref[n * heads + h].astype(f32)
            dp = mm_nt(dom, vw).astype(bf16).astype(f32)
            ds = p * (dp - jnp.sum(dp * p, -1, keepdims=True))
            if n == 0:
                bias_grad_ref[h] = ds
            else:
                bias_grad_ref[h] += ds
            dsb = (ds * factor).astype(bf16)
            a = mm(dsb, pick(masks[h], kw))
            b = mm_tn(dsb, pick(masks[h], qw))
            c = mm_tn(p.astype(bf16), dom)
            dq, dk, dv = (a, b, c) if dq is None else (dq + a, dk + b, dv + c)
        dqs.append(dq.astype(bf16))
        dks.append(dk.astype(bf16))
        dvs.append(dv.astype(bf16))
    dq, dk, dv = (jnp.concatenate(parts, 0) for parts in (dqs, dks, dvs))
    qkv_w = w_qkv[...]
    dn1 = None
    for i, part in enumerate((dq, dk, dv)):
        term = mm_nt(part, qkv_w[:, i * channels : (i + 1) * channels])
        dn1 = term if dn1 is None else dn1 + term
    dn1 = dn1.astype(bf16).astype(f32)
    du, gain_grad = norm_back(dn1, hat1, scale1, gains[0:1, :])
    return dmid + du, gain_grad, dq, dk, dv, dp_out


def attention_weights(n1, o, dq, dk, dv, dp_out):
    return [jnp.concatenate([mm_tn(n1, part) for part in (dq, dk, dv)], 1), mm_tn(o, dp_out)]


def mlp_weights(n2, g, dh, dz, lat):
    channels = n2.shape[1]
    groups = g.shape[1] // channels
    g_fc2 = mm_tn(g, dz).reshape(lat, groups, channels // lat, channels)
    return [mm_tn(n2, dh)] + [g_fc2[:, a].reshape(channels, channels) for a in range(groups)]


class Late:
    def __init__(self, copy, buffer):
        self.copy, self.buffer, self.here = copy, buffer, False

    def ready(self):
        if not self.here:
            self.copy.wait()
            self.here = True
        return self.buffer

    def __getitem__(self, index):
        return self.ready()[index]


class Sink:
    def __init__(self, copy, buffer):
        self.copy, self.buffer, self.sent = copy, buffer, False
        self.shape, self.dtype = buffer.shape, buffer.dtype

    def __getitem__(self, index):
        return self.buffer[index]

    def __setitem__(self, index, value):
        self.buffer[index] = value

    def send(self):
        if not self.sent:
            self.copy.start()
            self.sent = True


def call(fn, ins, outs, near, scratch, name, flops, limit, scalar=None):
    arrays = [array for array, _ in ins]
    picks = [index for _, index in ins]
    n_in, n_out, n_near = len(ins), len(outs), len(near)
    n_scalar = 0 if scalar is None else 1
    in_buffers = [pltpu.VMEM(a.shape if i is None else a.shape[1:], a.dtype) for a, i in ins]
    out_buffers = [pltpu.VMEM(o.shape, o.dtype) for o in outs]

    def kernel(*refs):
        refs = list(refs)

        def take(n):
            front = refs[:n]
            del refs[:n]
            return front

        scalars, sources, targets, nears = take(n_scalar), take(n_in), take(n_out), take(n_near)
        in_refs, out_refs, (in_sems, out_sems) = take(n_in), take(n_out), take(2)
        lates, sinks = [], []
        for i, (source, index, buffer) in enumerate(zip(sources, picks, in_refs)):
            copy = pltpu.make_async_copy(source if index is None else source.at[index], buffer, in_sems.at[i])
            copy.start()
            lates.append(Late(copy, buffer))
        for i, (target, buffer) in enumerate(zip(targets, out_refs)):
            sinks.append(Sink(pltpu.make_async_copy(buffer, target, out_sems.at[i]), buffer))
        fn(*scalars, lates, sinks, nears, refs)
        for late in lates:
            late.ready()
        for sink in sinks:
            sink.send()
        for sink in sinks:
            sink.copy.wait()

    hbm = pl.BlockSpec(memory_space=pltpu.HBM)
    vmem = pl.BlockSpec(memory_space=pltpu.VMEM)
    moved = sum(b.size * b.dtype.itemsize for b in [*arrays, *outs])
    with jax.named_scope("k_" + name):
        return pl.pallas_call(
            kernel,
            out_shape=[*outs, *near],
            in_specs=[pl.BlockSpec(memory_space=pltpu.SMEM)] * n_scalar + [hbm] * n_in,
            out_specs=[hbm] * n_out + [vmem] * n_near,
            scratch_shapes=in_buffers + out_buffers
            + [pltpu.SemaphoreType.DMA((n_in,)), pltpu.SemaphoreType.DMA((max(n_out, 1),))] + list(scratch),
            name=name,
            compiler_params=pltpu.CompilerParams(vmem_limit_bytes=limit * 1024 * 1024),
            cost_estimate=pl.CostEstimate(flops=flops, bytes_accessed=moved, transcendentals=0),
        )(*([] if scalar is None else [scalar]), *arrays)


def put_norm(ref, hat, scale):
    channels = hat.shape[1]
    ref[:, :channels] = hat
    ref[:, channels : channels + 1] = scale


def get_norm(ref, channels):
    value = ref[...]
    return value[:, :channels], value[:, channels : channels + 1]


def send_messages(value, chosen, messages):
    for message, choice in zip(messages, chosen):
        message[...] = mm(choice[...], value).astype(bf16)


def join(parts, choices):
    total = None
    for part, choice in zip(parts, choices):
        term = mm(choice[...], part[...])
        total = term if total is None else total + term
    return total


def first_kernel(plan, ins, outs, near, scratch):
    table, row_pick, lane_pick, x, to_order, w_qkv, gains, w_proj, w_fc1, w_fc2, cot, *chosen = ins
    s1, p_out, norm1, q_out, k_out, v_out, o_out, norm2, slope_out, g_out = outs
    rows_ref, x_ref, bias_ref = scratch
    expand_bias(table, row_pick, lane_pick, rows_ref, x_ref, bias_ref, plan.heads, None)
    u = mm(to_order[...], x[...])
    n1, hat1, scale1, q, k, v, o, middle, n2, hat2, scale2, wide, cdf, g = forward(
        u, gains, (w_qkv, w_proj, w_fc1), bias_ref, p_out, plan)
    put_norm(norm1, hat1, scale1)
    put_norm(norm2, hat2, scale2)
    for ref, value in ((q_out, q), (k_out, k), (v_out, v), (o_out, o), (slope_out, slope(wide, cdf).astype(bf16)), (g_out, g)):
        ref[...] = value
    for ref in outs[1:]:
        ref.send()
    out = middle + mm_nt(g, w_fc2[...])
    both = jnp.concatenate([out, mm(to_order[...], cot[...])], 1).astype(bf16)
    send_messages(both, chosen, near)
    s1[...] = both


def between_kernel(plan, last, ins, outs, near, scratch):
    table, row_pick, lane_pick, level_mask, late_mask = ins
    mask = level_mask[...] + late_mask[...] * last[0].astype(f32)
    expand_bias(table, row_pick, lane_pick, *scratch, outs[0], plan.heads, mask)


def sides(mine):
    return 1 - mine[0], mine[0]


def second_kernel(plan, board, mine, ins, outs, near, scratch):
    channels = plan.channels
    s1, roll0, r_lat, r_lon, r_cor, roll1, roll2, roll3, w_qkv, gains, bias, w_proj, w_fc1, w_fc2, *chosen = ins[:-2]
    row_pick, lane_pick = ins[-2:]
    rolled, keep, send = outs
    p_ref, bias_grad, fold_ref, grads = scratch
    grads[:, board.table_at :, :] = jnp.zeros_like(grads[:, board.table_at :, :])
    both = join((s1, r_lat, r_lon, r_cor), (roll0, roll1, roll2, roll3))
    u, cot = both[:, :channels], both[:, channels:]
    n1, hat1, scale1, q, k, v, o, middle, n2, hat2, scale2, wide, cdf, g = forward(
        u, gains, (w_qkv, w_proj, w_fc1), bias, p_ref, plan)
    dmid, gain_two, dz, dh = mlp_back(cot, gains, (w_fc1, w_fc2), hat2, scale2, slope(wide, cdf))
    du, gain_one, dq, dk, dv, dp_out = attention_back(
        dmid, gains, (w_qkv, w_proj), hat1, scale1, q, k, v, p_ref, bias_grad, plan)
    du = du.astype(bf16)
    rolled[...] = du
    rolled.send()
    send_messages(du, chosen, near)
    side = sides(mine)
    parts = attention_weights(n1, o, dq, dk, dv, dp_out) + mlp_weights(n2, g, dh, dz, board.lats)
    board.put_slices(grads, side, parts)
    board.put_gains(grads, (gain_one, gain_two))
    board.put_table(grads, side, fold_bias(bias_grad, row_pick, lane_pick, fold_ref, plan.heads), plan.heads)
    send[...] = grads[0].astype(bf16)
    send.send()
    keep[...] = grads[1].astype(bf16)


def third_kernel(plan, board, mine, ins, outs, near, scratch):
    rolled, r_lat, r_lon, r_cor, unroll0, unroll1, unroll2, unroll3, w_fc2, gelu_slope, w_fc1, norm2, gains, g = ins[:14]
    w_proj, v, p, k, q, w_qkv, norm1, o, to_natural, row_pick, lane_pick = ins[14:]
    send, keep, state_grad = outs
    bias_grad, fold_ref, grads = scratch
    grads[:, board.table_at :, :] = jnp.zeros_like(grads[:, board.table_at :, :])
    grad = join((rolled, r_lat, r_lon, r_cor), (unroll0, unroll1, unroll2, unroll3))
    hat2, scale2 = get_norm(norm2, plan.channels)
    dmid, gain_two, dz, dh = mlp_back(grad, gains, (w_fc1, w_fc2), hat2, scale2, gelu_slope[...].astype(f32))
    hat1, scale1 = get_norm(norm1, plan.channels)
    du, gain_one, dq, dk, dv, dp_out = attention_back(
        dmid, gains, (w_qkv, w_proj), hat1, scale1, q[...], k[...], v[...], p, bias_grad, plan)
    state_grad[...] = sum(mm(to_natural[...], part) for part in split3(du))
    state_grad.send()
    side = sides(mine)
    n1 = (hat1 * gains[0:1, :]).astype(bf16)
    n2 = (hat2 * gains[1:2, :]).astype(bf16)
    parts = attention_weights(n1, o[...], dq, dk, dv, dp_out) + mlp_weights(n2, g[...], dh, dz, board.lats)
    board.put_slices(grads, side, parts)
    board.put_gains(grads, (gain_one, gain_two))
    board.put_table(grads, side, fold_bias(bias_grad, row_pick, lane_pick, fold_ref, plan.heads), plan.heads)
    send[...] = grads[0].astype(bf16)
    send.send()
    keep[...] = grads[1].astype(bf16)


def last_kernel(board, widths, heads, ins, outs, near, scratch):
    w_qkv, w_proj, w_fc1, w_fc2 = widths
    own, one, two, three, table_one, table_two = ins
    qkv, proj, fc1, fc2, gain_out, table_out = near
    rows, width = board.rows, board.width
    pieces = [part[...].astype(f32) for part in (own, one, two, three)]
    whole = (pieces[0][:rows] + pieces[1][:rows]) + (pieces[2][:rows] + pieces[3][:rows])
    gains = []
    count = 2 * board.gain_segments
    for piece in pieces:
        gains.append(piece[rows : rows + count] + piece[rows + count : rows + 2 * count])
    gain = (gains[0] + gains[1]) + (gains[2] + gains[3])
    for b, table in enumerate((table_one, table_two)):
        start = b * width
        for n in range(2):
            for segment in range(board.gain_segments):
                low = segment * width
                high = min(board.channels, low + width)
                row = n * board.gain_segments + segment
                gain_out[b, n : n + 1, low:high] = gain[row : row + 1, start : start + high - low]
        qkv[b] = whole[:, start : start + w_qkv]
        start += w_qkv
        proj[b] = whole[:, start : start + w_proj]
        start += w_proj
        fc1[b] = whole[:, start : start + w_fc1]
        start += w_fc1
        groups = (width - w_qkv - w_proj - w_fc1) // w_fc2
        tall = jnp.concatenate([whole[:, start + w_fc2 * a : start + w_fc2 * (a + 1)] for a in range(groups)], 0)
        fc2[b] = tall.T
        value = table[...].astype(f32)
        for segment in range(board.segments):
            low = segment * width
            high = min(board.chunk, low + width)
            for h in range(heads):
                table_out[b, h, :, low:high] = value[8 * segment + h : 8 * segment + h + 1, : high - low]


def rounded(v):
    return lax.reduce_precision(v, 8, 7)


def body(state, out_cot, qkv_weight, proj_weight, fc1_weight, fc2_weight, norm_gain, bias_table):
    levels, rows, lon, channels = state.shape
    heads = bias_table.shape[3]
    assert levels == WZ and rows == WH and lon % WW == 0
    plan = Plan(lon, heads, channels)
    tokens, windows = plan.tokens, plan.windows
    lats, lons = lax.axis_size("lat"), lax.axis_size("lon")
    count = lats * lons
    axes = ("lat", "lon")
    lat, lon_at = lax.axis_index("lat"), lax.axis_index("lon")
    me = lat * lons + lon_at

    def shift(value, by_lat, by_lon, scope):
        pairs = []
        for a in range(lats):
            for b in range(lons):
                pairs.append((a * lons + b, ((a + by_lat) % lats) * lons + (b + by_lon) % lons))
        with jax.named_scope(scope):
            return lax.ppermute(value, axes, pairs)

    def shape(*dims, kind=bf16):
        return jax.ShapeDtypeStruct(dims, kind)

    def whole(*arrays):
        return [(array, None) for array in arrays]

    x = state.reshape(tokens, channels)
    cot = out_cot.reshape(tokens, channels)
    entries = bias_table.shape[-1]
    table = bias_table.reshape(2, heads, 1, entries)
    w_qkv, w_proj, w_fc1 = qkv_weight, proj_weight, fc1_weight
    w_fc2 = fc2_weight.transpose(0, 2, 1)
    weights = (w_qkv, w_proj, w_fc1, w_fc2)
    hidden = fc1_weight.shape[-1]
    groups = hidden // channels
    widths = tuple(w.shape[-1] // lons for w in (w_qkv, w_proj, w_fc1)) + (channels // lons,)
    part_a = widths[0] + widths[1]
    part_b = widths[2] + groups * widths[3]
    width = part_a + part_b
    board = Board(lats, lons, channels, width, entries)
    bias_shape = shape(heads, WT, WT, kind=f32)
    expand_scratch = [pltpu.VMEM((8, entries), f32), pltpu.VMEM((8 * ZH, 512), f32)]
    bias_scratch = pltpu.VMEM(bias_shape.shape, f32)
    fold_scratch = pltpu.VMEM((16 * heads, 384), f32)
    board_scratch = pltpu.VMEM((2, board.total, width), f32)
    board_shape = shape(board.total, width)
    wide_f32 = shape(tokens, channels, kind=f32)
    norm_shape = shape(tokens, 128 * (channels // 128 + 1), kind=f32)
    narrow = shape(tokens, channels)
    hidden_bf16 = shape(tokens, hidden)
    picks = whole(plan.row_pick, plan.lane_pick)
    mine = (me & 1).reshape(1)

    def messages(wide):
        return [shape(n, wide) for n in plan.sizes]

    flops = 2 * tokens * sum(w.size // 2 for w in weights)
    s1, p, norm1, q, k, v, o, norm2, gelu_slope, g, m_lat, m_lon, m_cor = call(
        functools.partial(first_kernel, plan),
        [(table, 0), *picks, *whole(x, plan.to_order), (w_qkv, 0), (norm_gain, 0), (w_proj, 0), (w_fc1, 0), (w_fc2, 0),
         *whole(cot, *plan.send_down)],
        [shape(tokens, 2 * channels), shape(windows * heads, WT, WT), norm_shape, narrow, narrow, narrow, narrow, norm_shape,
         hidden_bf16, hidden_bf16],
        messages(2 * channels),
        expand_scratch + [bias_scratch],
        "first", flops, LIMIT,
    )
    r_lat = shift(m_lat, -1, 0, "x1_lat")
    r_lon = shift(m_lon, 0, -1, "x1_lon")
    r_cor = shift(m_cor, -1, -1, "x1_cor")
    last = (lat == lats - 1).astype(jnp.int32).reshape(1)
    (bias_two,) = call(
        functools.partial(between_kernel, plan),
        [(table, 1), *picks, *whole(plan.level_mask, plan.late_mask)],
        [bias_shape], [], expand_scratch, "between", flops, LIMIT, last,
    )
    rolled, keep_two, send_two, m_lat, m_lon, m_cor = call(
        functools.partial(second_kernel, plan, board),
        [*whole(s1, plan.roll[0], r_lat, r_lon, r_cor, *plan.roll[1:]), (w_qkv, 1), (norm_gain, 1), *whole(bias_two),
         (w_proj, 1), (w_fc1, 1), (w_fc2, 1), *whole(*plan.send_up), *picks],
        [narrow, board_shape, board_shape],
        messages(channels),
        [pltpu.VMEM((windows * heads, WT, WT), f32), bias_scratch, fold_scratch, board_scratch],
        "second", 2 * flops, LIMIT, mine,
    )
    r_lat = shift(m_lat, 1, 0, "x2_lat")
    r_lon = shift(m_lon, 0, 1, "x2_lon")
    r_cor = shift(m_cor, 1, 1, "x2_cor")
    send_one, keep_one, state_grad = call(
        functools.partial(third_kernel, plan, board),
        [*whole(rolled, r_lat, r_lon, r_cor, *plan.unroll), (w_fc2, 0), *whole(gelu_slope), (w_fc1, 0), *whole(norm2),
         (norm_gain, 0), *whole(g), (w_proj, 0), *whole(v, p, k, q), (w_qkv, 0), *whole(norm1, o, plan.to_natural), *picks],
        [board_shape, board_shape, wide_f32], [],
        [bias_scratch, fold_scratch, board_scratch], "third", 2 * flops, LIMIT, mine,
    )

    bits = count.bit_length() - 1
    lon_bits = lons.bit_length() - 1
    gain_rows = 2 * board.gain_segments

    def exchange(value, mask, scope):
        with jax.named_scope(scope):
            return lax.ppermute(value, axes, [(i, i ^ mask) for i in range(count)])

    def part(held, at):
        return lax.dynamic_index_in_dim(held, at, held.ndim - 3, keepdims=False)

    def flat(value):
        return value.reshape(-1, value.shape[-1])

    def pack_gain(gain):
        high = rounded(gain)
        low = rounded(gain - high)
        both = jnp.concatenate((high, low, jnp.zeros((8 - 2 * gain_rows, gain.shape[-1]), f32)), 0)
        return high + low, both.astype(bf16)

    def unpack_gain(got):
        got = got.astype(f32)
        return got[:gain_rows] + got[gain_rows : 2 * gain_rows]

    def begin(send, keep, scope):
        got = exchange(send, 1, scope)
        table, gain = board.table_at, board.gain_at
        total = (keep[:gain].astype(f32) + got[:gain].astype(f32)).astype(bf16)
        slices = total[:table].reshape((2,) * (bits - 1) + (board.rows, width))
        tables = total[table:].reshape((2,) * (lon_bits - 1) + (8 * board.segments, width))
        return slices, tables, unpack_gain(keep[gain:]) + unpack_gain(got[gain:])

    def advance(held, bit, scope):
        slices, tables, gain = held
        at = (me >> bit) & 1
        gain, extra = pack_gain(gain)
        send = flat(part(slices, 1 - at))
        pieces = [send, extra]
        with_table = bit < lon_bits
        if with_table:
            pieces.append(flat(part(tables, 1 - at)))
        got = exchange(jnp.concatenate(pieces, 0), 1 << bit, scope)
        size = send.shape[0]
        keep = part(slices, at)
        slices = (keep.astype(f32) + got[:size].reshape(keep.shape).astype(f32)).astype(bf16)
        gain = gain + unpack_gain(got[size : size + 8])
        if with_table:
            keep = part(tables, at)
            tables = keep.astype(f32) + got[size + 8 :].reshape(keep.shape).astype(f32)
            if bit < lon_bits - 1:
                tables = tables.astype(bf16)
        return slices, tables, gain

    two = begin(send_two, keep_two, "two_0")
    one = begin(send_one, keep_one, "one_0")
    for bit in range(1, bits - 2):
        two = advance(two, bit, "two_%d" % bit)
        one = advance(one, bit, "one_%d" % bit)
    slices = jnp.concatenate((one[0], two[0]), -1).reshape(4, board.rows, 2 * width)
    _, extra = pack_gain(jnp.concatenate((one[2], two[2]), -1))
    high = me >> (bits - 2)

    def message(step):
        return jnp.concatenate((part(slices, high ^ step), extra), 0)

    got = [exchange(message(step), step << (bits - 2), "high_%d" % step) for step in (1, 2, 3)]
    qkv, proj, fc1, fc2, gain, tables = call(
        functools.partial(last_kernel, board, widths, heads),
        whole(message(0), *got, one[1], two[1]), [],
        [shape(2, board.rows, n, kind=f32) for n in widths[:3]]
        + [shape(2, widths[3], groups * board.rows, kind=f32), shape(2, 2, channels, kind=f32),
           shape(2, heads, 1, board.chunk, kind=f32)],
        [], "last", 1000, 8,
    )
    return (
        state_grad.reshape(state.shape),
        qkv,
        proj,
        fc1,
        fc2.transpose(0, 2, 1),
        gain,
        tables.reshape(2, 1, 1, heads, -1),
    )


LIMIT = 60


def solution(mesh):
    in_specs = (
        P(None, "lat", "lon", None),
        P(None, "lat", "lon", None),
        P(),
        P(),
        P(),
        P(),
        P(),
        P(None, "lat", None, None, None),
    )
    out_specs = (
        P(None, "lat", "lon", None),
        P(None, "lat", "lon"),
        P(None, "lat", "lon"),
        P(None, "lat", "lon"),
        P(None, "lat", "lon"),
        P(),
        P(None, "lat", None, None, "lon"),
    )
    return jax.shard_map(body, mesh=mesh, in_specs=in_specs, out_specs=out_specs, check_vma=False)
```
